128 devices in a mesh: ty: 8 (over x, core), tx: 16 (over y, z).
Axes of the slice: x: 4, y: 4, z: 4, core: 2. Of those that a mesh axis runs over, the one named last changes fastest.
Arguments:
- potential_warmth: float32 [16, 1024, 8192], P(None, ('ty', 'tx')), may hold values from -2 to 30
- saltiness_field: float32 [16, 1024, 8192], P(None, ('ty', 'tx')), may hold values from 30 to 38
- ocean_tier_tally: int32 [1024, 8192], P(('ty', 'tx')), may hold values from 0 to 16, as said below
Outputs:
- buoyancy_anomaly: float32 [16, 1024, 8192], P(None, 'ty', 'tx')
- laplacian: float32 [16, 1024, 8192], P(None, 'ty', 'tx')
The draws below stay inside these ranges and needn't reach their ends.
Inputs may be any that keep to these rules, and one draw needn't show every extreme that they name: `ocean_tier_tally`: columns with 0 are land; the tile of rows 0 .. 127 and columns 0 .. 511 is land in every draw, and other whole tiles of land occur. Within the rows of one device and the columns of one tile, at most 3072 columns are ocean, and some such block has exactly 3072.
All inputs are finite; a program needn't handle non-finite values.
Results may differ from the reference program's by a relative error of at most 0.00002.
Values sent between devices are 32-bit elements; how exact they have to be, the bound alone decides.
A program may use at most 128 MiB of HBM per device.

```python
import jax
import jax.numpy as jnp

SOUNDING_TIERS = 16
CJ = 128
CI = 512
MESH_PARALLELS = 1024
MESH_MERIDIANS = 8192
BAND = 8
OCEAN_COLS = 3072


def draw_ocean_tier_tally(key, part):
    first_key, second_key, third_key, fourth_key, fifth_key = jax.random.split(key, 5)
    tile_rows = MESH_PARALLELS // CJ
    tile_cols = MESH_MERIDIANS // CI
    groups = MESH_PARALLELS // BAND
    land_tiles = jax.random.randint(first_key, (tile_rows, tile_cols), 0, 4) == 0
    land_tiles = land_tiles.at[0, 0].set(True)
    land_tiles = land_tiles.at[tile_rows - 1, tile_cols - 1].set(False)
    scores = jax.random.randint(fourth_key, (groups, BAND, tile_cols, CI), 0, 1 << 30)
    scores = jnp.transpose(scores, (0, 2, 1, 3)).reshape(groups, tile_cols, BAND * CI)
    ranks = jnp.argsort(jnp.argsort(scores, axis=2, stable=True), axis=2, stable=True)
    counts = jax.random.randint(fifth_key, (groups, tile_cols), OCEAN_COLS // 2, OCEAN_COLS + 1)
    counts = counts.at[groups - 1, tile_cols - 1].set(OCEAN_COLS)
    ocean_cols = ranks < counts[:, :, None]
    ocean_cols = jnp.transpose(ocean_cols.reshape(groups, tile_cols, BAND, CI), (0, 2, 1, 3)).reshape(MESH_PARALLELS, MESH_MERIDIANS)
    levels_drawn = jax.random.randint(second_key, (MESH_PARALLELS, MESH_MERIDIANS), 1, SOUNDING_TIERS + 1)
    full_depth = jax.random.randint(third_key, (MESH_PARALLELS, MESH_MERIDIANS), 0, 2)
    levels_drawn = jnp.where(full_depth == 1, SOUNDING_TIERS, levels_drawn)
    land_cells = jnp.repeat(jnp.repeat(land_tiles, CJ, 0), CI, 1)
    keep = jnp.logical_and(ocean_cols, jnp.logical_not(land_cells))
    return jnp.where(keep, levels_drawn, 0).astype(jnp.int32)


def shard_levels(key, shape, cuts, least, largest):
    factor_of, own = 1.0, jax.random.fold_in(key, 6)
    for dim, shards_of in cuts:
        draws = jnp.exp(jax.random.uniform(jax.random.fold_in(own, dim), (shards_of,), jnp.float32, least / len(cuts), largest / len(cuts)))
        factor_of = factor_of * jnp.repeat(draws, shape[dim] // shards_of).reshape([-1 if axis == dim else 1 for axis in range(len(shape))])
    return factor_of


def setup_inputs(seed: int = 0) -> dict:
    key_of = jax.random.split(jax.random.key(seed), 4)
    return {
        "potential_warmth": jnp.clip(-2.0 + 32.0 * jax.random.uniform(key_of[0], (SOUNDING_TIERS, MESH_PARALLELS, MESH_MERIDIANS), jnp.float32) ** shard_levels(key_of[0], (SOUNDING_TIERS, MESH_PARALLELS, MESH_MERIDIANS), ((1, 128),), -0.2, 0.2), -2.0, 30.0),
        "saltiness_field": jnp.clip(30.0 + 8.0 * jax.random.uniform(key_of[1], (SOUNDING_TIERS, MESH_PARALLELS, MESH_MERIDIANS), jnp.float32) ** shard_levels(key_of[1], (SOUNDING_TIERS, MESH_PARALLELS, MESH_MERIDIANS), ((1, 128),), -0.2, 0.2), 30.0, 38.0),
        "ocean_tier_tally": draw_ocean_tier_tally(jax.random.fold_in(key_of[3], 71), 0),
    }


therm_coef = 0.16550
haline_coef = 0.76554
cabbel_coef = 0.059520
haline_second = 0.00054914
thermo_press = 0.00014970
haline_press = 0.000011090
cross_coef = 0.0024341


def ocean_properties(potential_warmth, saltiness_field, wet_indicator, sounding_tiers_list):
    heat_properties = potential_warmth - 10.0
    haline = saltiness_field - 35.0
    height = sounding_tiers_list[:, None, None]
    anomaly = -therm_coef * (1.0 + 0.5 * cabbel_coef * heat_properties + thermo_press * height) * heat_properties
    anomaly = anomaly + haline_coef * (1.0 - 0.5 * haline_second * haline - haline_press * height) * haline
    anomaly = anomaly - cross_coef * heat_properties * haline
    return wet_indicator * anomaly


def reference(potential_warmth, saltiness_field, ocean_tier_tally):
    level_index = jnp.arange(SOUNDING_TIERS, dtype=jnp.int32)
    wet_indicator = (level_index[:, None, None] < ocean_tier_tally[None]).astype(jnp.float32)
    sounding_tiers_list = 5.0 + 10.0 * jnp.arange(SOUNDING_TIERS, dtype=jnp.float32)
    buoyancy_anomaly = ocean_properties(potential_warmth, saltiness_field, wet_indicator, sounding_tiers_list)
    north_density = jnp.concatenate([buoyancy_anomaly[:, 1:, :], buoyancy_anomaly[:, -1:, ::-1]], 1)
    north_ocean = jnp.concatenate([wet_indicator[:, 1:, :], wet_indicator[:, -1:, ::-1]], 1)
    south_density = jnp.concatenate([jnp.zeros_like(buoyancy_anomaly[:, :1]), buoyancy_anomaly[:, :-1]], 1)
    south_ocean = jnp.concatenate([jnp.zeros_like(wet_indicator[:, :1]), wet_indicator[:, :-1]], 1)
    east_density = jnp.roll(buoyancy_anomaly, -1, 2)
    east_ocean = jnp.roll(wet_indicator, -1, 2)
    west_density = jnp.roll(buoyancy_anomaly, 1, 2)
    west_ocean = jnp.roll(wet_indicator, 1, 2)
    laplacian = north_ocean * (north_density - buoyancy_anomaly) + south_ocean * (south_density - buoyancy_anomaly)
    laplacian = laplacian + east_ocean * (east_density - buoyancy_anomaly) + west_ocean * (west_density - buoyancy_anomaly)
    return buoyancy_anomaly, wet_indicator * laplacian
```

```python
import functools

import jax
import jax.numpy as jnp
from jax import lax
from jax.experimental import pallas as pl
from jax.experimental.pallas import tpu as pltpu
from jax.sharding import PartitionSpec as P

therm_coef = 0.1655
haline_coef = 0.76554
cabbel_coef = 0.05952
haline_second = 0.00054914
thermo_press = 0.0001497
haline_press = 1.109e-05
cross_coef = 0.0024341

MESH = pl.DeviceIdType.MESH
TIERS = 16
BAND = 8
CJ = 128
CI = 512
NX = 16
NY = 8
COLS = NX * CI
CHUNKS = 4
PER = TIERS // CHUNKS
FAR = ((2, 2), (2, 1), (2, 3), (1, 2), (3, 2), (1, 1), (3, 3), (1, 3), (3, 1), (2, 0), (0, 2), (1, 0), (3, 0), (0, 1), (0, 3), (0, 0))


def density(warmth, salt, tally, tier):
    depth = 5.0 + 10.0 * tier
    a = warmth - 10.0
    b = salt - 35.0
    heat = (-therm_coef * (1.0 + thermo_press * depth)) - (0.5 * therm_coef * cabbel_coef) * a - cross_coef * b
    salty = (haline_coef * (1.0 - haline_press * depth)) - (0.5 * haline_coef * haline_second) * b
    return jnp.where(tally > tier, heat * a + salty * b, 0.0)


def partner_of(tx, step):
    dy = jnp.int32(0)
    dz = jnp.int32(0)
    for number, (far_y, far_z) in enumerate(FAR):
        dy = jnp.where(step == number, far_y, dy)
        dz = jnp.where(step == number, far_z, dz)
    return lax.rem(tx // 4 + dy, 4) * 4 + lax.rem(lax.rem(tx, 4) + dz, 4)


def exchange(
    warmth, salt, tally, tiles, rims, south, north,
    heat, brine, bottom, send, rim_low, rim_high, rim_send,
    in_sem, send_sem, recv_sem, rim_ssem, rim_rsem, own_sem, row_ssem, row_rsem,
):
    ty = lax.axis_index("ty")
    tx = lax.axis_index("tx")
    barrier = pltpu.get_barrier_semaphore()
    loads = [pltpu.make_async_copy(tally, bottom, in_sem.at[2 * CHUNKS])]
    for chunk in range(CHUNKS):
        part = pl.ds(chunk * PER, PER)
        loads.append(pltpu.make_async_copy(warmth.at[part], heat.at[part], in_sem.at[2 * chunk]))
        loads.append(pltpu.make_async_copy(salt.at[part], brine.at[part], in_sem.at[2 * chunk + 1]))
    for load in loads:
        load.start()
    for step in range(1, NX):
        pl.semaphore_signal(barrier, inc=1, device_id={"tx": lax.rem(tx + step, NX)}, device_id_type=MESH)

    @pl.when(ty > 0)
    def _():
        pl.semaphore_signal(barrier, inc=1, device_id={"ty": ty - 1}, device_id_type=MESH)

    @pl.when(ty < NY - 1)
    def _():
        pl.semaphore_signal(barrier, inc=1, device_id={"ty": ty + 1}, device_id_type=MESH)

    neighbours = jnp.where(ty > 0, 1, 0) + jnp.where(ty < NY - 1, 1, 0)
    pl.semaphore_wait(barrier, NX - 1 + neighbours)
    loads[0].wait()

    lanes = lax.broadcasted_iota(jnp.int32, (BAND, 128), 1)
    my_rows = pl.ds(pl.multiple_of(tx * BAND, BAND), BAND)

    def part_of(chunk):
        return pl.ds(0, PER + 1) if chunk == 0 else pl.ds(1 + chunk * PER, PER)

    def block_copy(chunk, step):
        to = partner_of(tx, step)
        return pltpu.make_async_remote_copy(
            src_ref=send.at[to, part_of(chunk)],
            dst_ref=tiles.at[part_of(chunk), my_rows],
            send_sem=send_sem.at[chunk, to],
            recv_sem=recv_sem.at[chunk, tx],
            device_id={"tx": to},
            device_id_type=MESH,
        )

    def arrival(chunk, source):
        rows = pl.ds(pl.multiple_of(source * BAND, BAND), BAND)
        return pltpu.make_async_remote_copy(
            src_ref=send.at[source, part_of(chunk)],
            dst_ref=tiles.at[part_of(chunk), rows],
            send_sem=send_sem.at[chunk, source],
            recv_sem=recv_sem.at[chunk, source],
            device_id={"tx": source},
            device_id_type=MESH,
        )

    for chunk in range(CHUNKS):
        loads[1 + 2 * chunk].wait()
        loads[2 + 2 * chunk].wait()

        def make(step, carry, chunk=chunk):
            to = partner_of(tx, step)
            at = pl.ds(pl.multiple_of(to * CI, CI), CI)
            deep = bottom[:, at]
            low = jnp.zeros((BAND, 128), jnp.float32)
            high = jnp.zeros((BAND, 128), jnp.float32)
            for tier in range(chunk * PER, chunk * PER + PER):
                value = density(heat[tier, :, at], brine[tier, :, at], deep, tier)
                send[to, 1 + tier] = value
                low = jnp.where(lanes == tier, pltpu.roll(value[:, CI - 128 :], (tier + 1) % 128, 1), low)
                high = jnp.where(lanes == 32 + tier, pltpu.roll(value[:, :128], 32 + tier, 1), high)
            if chunk == 0:
                deep = deep.astype(jnp.float32)
                send[to, 0] = deep
                low = jnp.where(lanes == TIERS, pltpu.roll(deep[:, CI - 128 :], TIERS + 1, 1), low)
                high = jnp.where(lanes == 32 + TIERS, pltpu.roll(deep[:, :128], 32 + TIERS, 1), high)
                rim_low[lax.rem(to + 1, NX)] = low
                rim_high[lax.rem(to + NX - 1, NX)] = high
            else:
                east = lax.rem(to + 1, NX)
                west = lax.rem(to + NX - 1, NX)
                rim_low[east] = rim_low[east] + low
                rim_high[west] = rim_high[west] + high

            @pl.when(step > 0)
            def _():
                block_copy(chunk, step - 1).start()

            return carry

        lax.fori_loop(0, NX, make, 0)

    own = pltpu.make_async_copy(send.at[tx], tiles.at[:, my_rows], own_sem.at[0])
    own.start()

    def join(step, carry):
        to = partner_of(tx, step)
        rim_send[to] = rim_low[to] + rim_high[to]
        return carry

    lax.fori_loop(0, NX, join, 0)

    def rim_copy(to):
        return pltpu.make_async_remote_copy(
            src_ref=rim_send.at[to],
            dst_ref=rims.at[my_rows],
            send_sem=rim_ssem.at[to],
            recv_sem=rim_rsem.at[tx],
            device_id={"tx": to},
            device_id_type=MESH,
        )

    def rim_arrival(source):
        rows = pl.ds(pl.multiple_of(source * BAND, BAND), BAND)
        return pltpu.make_async_remote_copy(
            src_ref=rim_send.at[source],
            dst_ref=rims.at[rows],
            send_sem=rim_ssem.at[source],
            recv_sem=rim_rsem.at[source],
            device_id={"tx": source},
            device_id_type=MESH,
        )

    def send_rim(step, carry):
        rim_copy(partner_of(tx, step)).start()
        return carry

    lax.fori_loop(0, NX - 1, send_rim, 0)
    own_rim = pltpu.make_async_copy(rim_send.at[tx], rims.at[my_rows], own_sem.at[1])
    own_rim.start()
    own.wait()

    def band_in(source):
        @pl.when(tx != source)
        def _():
            for chunk in range(CHUNKS):
                arrival(chunk, source).wait_recv()

    first = pl.ds(0, BAND)
    last = pl.ds(CJ - BAND, BAND)
    downward = pltpu.make_async_remote_copy(
        src_ref=tiles.at[:, first], dst_ref=north, send_sem=row_ssem.at[0], recv_sem=row_rsem.at[0],
        device_id={"ty": jnp.maximum(ty - 1, 0)}, device_id_type=MESH,
    )
    upward = pltpu.make_async_remote_copy(
        src_ref=tiles.at[:, last], dst_ref=south, send_sem=row_ssem.at[1], recv_sem=row_rsem.at[1],
        device_id={"ty": jnp.minimum(ty + 1, NY - 1)}, device_id_type=MESH,
    )
    across = pltpu.make_async_remote_copy(
        src_ref=tiles.at[:, last], dst_ref=north, send_sem=row_ssem.at[1], recv_sem=row_rsem.at[0],
        device_id={"tx": NX - 1 - tx}, device_id_type=MESH,
    )
    band_in(0)

    @pl.when(ty > 0)
    def _():
        downward.start()

    band_in(NX - 1)

    @pl.when(ty < NY - 1)
    def _():
        upward.start()

    @pl.when(ty == NY - 1)
    def _():
        across.start()

    def gather_in(source, carry):
        @pl.when(source != tx)
        def _():
            rim_arrival(source).wait_recv()
            rim_copy(source).wait_send()
            for chunk in range(CHUNKS):
                @pl.when(jnp.logical_and(source > 0, source < NX - 1))
                def _():
                    arrival(chunk, source).wait_recv()

                arrival(chunk, source).wait_send()

        return carry

    lax.fori_loop(0, NX, gather_in, 0)
    own_rim.wait()

    @pl.when(ty > 0)
    def _():
        downward.wait_send()
        upward.wait_recv()

    @pl.when(ty < NY - 1)
    def _():
        upward.wait_send()
        downward.wait_recv()

    @pl.when(ty == NY - 1)
    def _():
        across.wait()


def stencil(place, tiles, bottom, rims, south, north, south_bottom, north_bottom, out, lap, edge_bottom):
    tier = pl.program_id(0)
    ty = place[0]
    rows = lax.broadcasted_iota(jnp.int32, (CJ, CI), 0)
    lanes = lax.broadcasted_iota(jnp.int32, (CJ, 128), 1)
    turn = 127 - lax.broadcasted_iota(jnp.int32, (BAND, 128), 1)

    def northern(ref):
        block = ref[0]
        pieces = [jnp.take_along_axis(block[:, 128 * p : 128 * p + 128], turn, axis=1) for p in (3, 2, 1, 0)]
        flipped = jnp.concatenate(pieces, axis=1)[BAND - 1 :]
        return jnp.where(ty == NY - 1, flipped, block[:1])

    def southern(ref):
        return jnp.where(ty > 0, ref[0][BAND - 1 :], 0.0)

    def beside(field, level, upper, lower):
        rim = rims[...]
        east = pltpu.roll(field, CI - 1, 1)
        west = pltpu.roll(field, 1, 1)
        east_rim = pltpu.roll(rim, lax.rem(127 - 32 - level + 128, 128), 1)
        west_rim = pltpu.roll(rim, lax.rem(128 - level, 128), 1)
        east = jnp.concatenate([east[:, : CI - 128], jnp.where(lanes == 127, east_rim, east[:, CI - 128 :])], 1)
        west = jnp.concatenate([jnp.where(lanes == 0, west_rim, west[:, :128]), west[:, 128:]], 1)
        up = jnp.where(rows == CJ - 1, upper, pltpu.roll(field, CJ - 1, 0))
        down = jnp.where(rows == 0, lower, pltpu.roll(field, 1, 0))
        return up, down, east, west

    @pl.when(tier == 0)
    def _():
        deep = bottom[0]
        around = beside(deep, TIERS, northern(north_bottom), southern(south_bottom))
        for side, other in enumerate(around):
            edge_bottom[side] = jnp.minimum(deep, other)

    field = tiles[0]
    out[0] = field
    level = tier.astype(jnp.float32)
    around = beside(field, tier, northern(north), southern(south))
    total = jnp.zeros((CJ, CI), jnp.float32)
    for side, other in enumerate(around):
        total = total + jnp.where(edge_bottom[side] > level, other - field, 0.0)
    lap[0] = total


def on_device(warmth, salt, tally):
    hbm = pl.BlockSpec(memory_space=pl.ANY)
    f32 = jnp.float32
    tiles, rims, south, north = pl.pallas_call(
        exchange,
        out_shape=(
            jax.ShapeDtypeStruct((TIERS + 1, CJ, CI), f32),
            jax.ShapeDtypeStruct((CJ, 128), f32),
            jax.ShapeDtypeStruct((TIERS + 1, BAND, CI), f32),
            jax.ShapeDtypeStruct((TIERS + 1, BAND, CI), f32),
        ),
        in_specs=[hbm] * 3,
        out_specs=(hbm,) * 4,
        scratch_shapes=[
            pltpu.VMEM((TIERS, BAND, COLS), f32),
            pltpu.VMEM((TIERS, BAND, COLS), f32),
            pltpu.VMEM((BAND, COLS), jnp.int32),
            pltpu.VMEM((NX, TIERS + 1, BAND, CI), f32),
            pltpu.VMEM((NX, BAND, 128), f32),
            pltpu.VMEM((NX, BAND, 128), f32),
            pltpu.VMEM((NX, BAND, 128), f32),
            pltpu.SemaphoreType.DMA((2 * CHUNKS + 1,)),
            pltpu.SemaphoreType.DMA((CHUNKS, NX)),
            pltpu.SemaphoreType.DMA((CHUNKS, NX)),
            pltpu.SemaphoreType.DMA((NX,)),
            pltpu.SemaphoreType.DMA((NX,)),
            pltpu.SemaphoreType.DMA((2,)),
            pltpu.SemaphoreType.DMA((2,)),
            pltpu.SemaphoreType.DMA((2,)),
        ],
        compiler_params=pltpu.CompilerParams(
            collective_id=0, has_side_effects=True, vmem_limit_bytes=40 * 2**20
        ),
        name="exchange",
    )(warmth, salt, tally)
    place = lax.axis_index("ty").astype(jnp.int32).reshape(1)
    level = lambda k, place: (k + 1, 0, 0)
    below = lambda k, place: (0, 0, 0)
    return pl.pallas_call(
        stencil,
        out_shape=(jax.ShapeDtypeStruct((TIERS, CJ, CI), f32),) * 2,
        grid_spec=pltpu.PrefetchScalarGridSpec(
            num_scalar_prefetch=1,
            grid=(TIERS,),
            in_specs=[
                pl.BlockSpec((1, CJ, CI), level),
                pl.BlockSpec((1, CJ, CI), below),
                pl.BlockSpec((CJ, 128), lambda k, place: (0, 0)),
                pl.BlockSpec((1, BAND, CI), level),
                pl.BlockSpec((1, BAND, CI), level),
                pl.BlockSpec((1, BAND, CI), below),
                pl.BlockSpec((1, BAND, CI), below),
            ],
            out_specs=[pl.BlockSpec((1, CJ, CI), lambda k, place: (k, 0, 0))] * 2,
            scratch_shapes=[pltpu.VMEM((4, CJ, CI), f32)],
        ),
        compiler_params=pltpu.CompilerParams(dimension_semantics=("arbitrary",)),
        name="stencil",
    )(place, tiles, tiles, rims, south, north, south, north)


def solution(mesh):
    placed = (P(None, ("ty", "tx"), None), P(None, ("ty", "tx"), None), P(("ty", "tx"), None))
    return jax.shard_map(
        on_device,
        mesh=mesh,
        in_specs=placed,
        out_specs=(P(None, "ty", "tx"), P(None, "ty", "tx")),
        check_vma=False,
    )
```

```python
import jax
import jax.numpy as jnp
from jax import lax
from jax.experimental import pallas as pl
from jax.experimental.pallas import tpu as pltpu
from jax.sharding import PartitionSpec as P

therm_coef = 0.1655
haline_coef = 0.76554
cabbel_coef = 0.05952
haline_second = 0.00054914
thermo_press = 0.0001497
haline_press = 1.109e-05
cross_coef = 0.0024341

MESH = pl.DeviceIdType.MESH
TIERS = 16
BAND = 8
CJ = 128
CI = 512
NX = 16
NY = 8
COLS = NX * CI
LANES = 128
ROWS = BAND * CI // LANES
KEPT = 24
SPARE = (ROWS - KEPT) * LANES
CUTS = (0, 4, 8, 12, 16)
CHUNKS = len(CUTS) - 1
PAD = BAND
FAR = ((2, 2), (2, 1), (2, 3), (1, 2), (3, 2), (1, 1), (3, 3), (1, 3), (3, 1), (2, 0), (0, 2), (1, 0), (3, 0), (0, 1), (0, 3), (0, 0))
f32 = jnp.float32
i32 = jnp.int32


def density(warmth, salt, tier):
    depth = 5.0 + 10.0 * tier
    a = warmth - 10.0
    b = salt - 35.0
    heat = (-therm_coef * (1.0 + thermo_press * depth)) - (0.5 * therm_coef * cabbel_coef) * a - cross_coef * b
    salty = (haline_coef * (1.0 - haline_press * depth)) - (0.5 * haline_coef * haline_second) * b
    return heat * a + salty * b


def partner_of(tx, step, sign=1):
    dy = jnp.int32(0)
    dz = jnp.int32(0)
    for number, (far_y, far_z) in enumerate(FAR):
        dy = jnp.where(step == number, far_y, dy)
        dz = jnp.where(step == number, far_z, dz)
    if sign < 0:
        dy, dz = 4 - dy, 4 - dz
    return lax.rem(tx // 4 + dy, 4) * 4 + lax.rem(lax.rem(tx, 4) + dz, 4)


def as_rows(block):
    return jnp.concatenate([block[:, LANES * v : LANES * v + LANES] for v in range(CI // LANES)], axis=0)


def as_block(rows):
    return jnp.concatenate([rows[BAND * v : BAND * v + BAND] for v in range(CI // LANES)], axis=1)


def land_counts(land):
    one = lax.broadcasted_iota(i32, (LANES, 2 * LANES), 0)
    two = lax.broadcasted_iota(i32, (LANES, 2 * LANES), 1)
    ahead = jnp.where(jnp.logical_or(two >= LANES, one < two), 1.0, 0.0).astype(jnp.bfloat16)
    both = jnp.dot(land.astype(jnp.bfloat16), ahead, preferred_element_type=f32)
    one = lax.broadcasted_iota(i32, (ROWS, ROWS), 0)
    two = lax.broadcasted_iota(i32, (ROWS, ROWS), 1)
    above = jnp.where(two < one, 1.0, 0.0).astype(jnp.bfloat16)
    start = jnp.dot(above, both[:, LANES:].astype(jnp.bfloat16), preferred_element_type=f32)
    cell = jnp.minimum(start + both[:, :LANES], float(SPARE))
    return jnp.minimum(start, float(SPARE)).astype(i32), cell.astype(i32)


def squeeze(state, bits, axis, roll):
    size = state.shape[axis]
    for bit in range(bits):
        flag = 256 << bit
        ahead = roll(state, size - (1 << bit), axis)
        stay = jnp.where((state & flag) != 0, 0, state)
        state = jnp.where((ahead & flag) != 0, ahead, stay)
    return state


def packing(tally, roll):
    start, cell = land_counts(jnp.where(tally > 0, 0.0, 1.0))
    lane = lax.broadcasted_iota(i32, (ROWS, LANES), 1)
    row = lax.broadcasted_iota(i32, (ROWS, LANES), 0)
    state = jnp.where(tally > 0, ((cell - start) << 8) | 128 | lane, 0)
    state = squeeze(state, 7, 1, roll) & 255
    state = jnp.take_along_axis(state, (lane + start) & 127, axis=1)
    back = (start + lane) >> 7
    rows = jnp.where(state >= 128, (back << 8) | row, 0)
    rows = squeeze(rows, 4, 0, roll) & 31
    return state & 127, rows[:KEPT]


def unpacking(tally):
    start, cell = land_counts(jnp.where(tally > 0, 0.0, 1.0))
    lane = lax.broadcasted_iota(i32, (ROWS, LANES), 1)
    row = lax.broadcasted_iota(i32, (ROWS, LANES), 0)
    return row - ((start + lane) >> 7), (lane - cell) & 127


def pack(rows, lane_from, row_from):
    moved = jnp.take_along_axis(rows, lane_from, axis=1)
    parts = []
    for w in range(KEPT // BAND):
        at = row_from[BAND * w : BAND * w + BAND]
        low = jnp.take_along_axis(moved[BAND * w : BAND * w + BAND], at & 7, axis=0)
        high = jnp.take_along_axis(moved[BAND * w + BAND : BAND * w + 2 * BAND], at & 7, axis=0)
        parts.append(jnp.where(at >= BAND * (w + 1), high, low))
    return jnp.concatenate(parts, axis=0)


def unpack(kept, row_from, lane_from):
    parts = []
    for v in range(ROWS // BAND):
        at = row_from[BAND * v : BAND * v + BAND]
        low = None if v == 0 else jnp.take_along_axis(kept[BAND * v - BAND : BAND * v], at & 7, axis=0)
        high = None if v == KEPT // BAND else jnp.take_along_axis(kept[BAND * v : BAND * v + BAND], at & 7, axis=0)
        if low is None or high is None:
            parts.append(high if low is None else low)
        else:
            parts.append(jnp.where(at >= BAND * v, high, low))
    return jnp.take_along_axis(jnp.concatenate(parts, axis=0), lane_from, axis=1)


def exchange(
    warmth, salt, tally, out, lap,
    heat, brine, bottom, boxes, deeps, depth, least, pack_lane, pack_row, rows_back, rim_low, rim_high, rims, rows_out, rows_in,
    in_sem, send_sem, recv_sem, rim_ssem, rim_rsem, row_ssem, row_rsem,
):
    ty = lax.axis_index("ty")
    tx = lax.axis_index("tx")
    barrier = pltpu.get_barrier_semaphore()
    loads = [pltpu.make_async_copy(tally, bottom, in_sem.at[2 * CHUNKS])]
    for chunk in range(CHUNKS):
        part = pl.ds(CUTS[chunk], CUTS[chunk + 1] - CUTS[chunk])
        loads.append(pltpu.make_async_copy(warmth.at[part], heat.at[part], in_sem.at[2 * chunk]))
        loads.append(pltpu.make_async_copy(salt.at[part], brine.at[part], in_sem.at[2 * chunk + 1]))
    for load in loads:
        load.start()
    for step in range(1, NX):
        pl.semaphore_signal(barrier, inc=1, device_id={"tx": lax.rem(tx + step, NX)}, device_id_type=MESH)

    @pl.when(ty > 0)
    def _():
        pl.semaphore_signal(barrier, inc=1, device_id={"ty": ty - 1}, device_id_type=MESH)

    @pl.when(ty < NY - 1)
    def _():
        pl.semaphore_signal(barrier, inc=1, device_id={"ty": ty + 1}, device_id_type=MESH)

    lanes = lax.broadcasted_iota(i32, (BAND, LANES), 1)

    def levels(chunk):
        return pl.ds(CUTS[chunk], CUTS[chunk + 1] - CUTS[chunk])

    def box_copy(chunk, to, source):
        return pltpu.make_async_remote_copy(
            src_ref=boxes.at[to, levels(chunk)], dst_ref=boxes.at[NX + source, levels(chunk)],
            send_sem=send_sem.at[chunk, to], recv_sem=recv_sem.at[chunk, source],
            device_id={"tx": to}, device_id_type=MESH,
        )

    def deep_copy(to, source):
        return pltpu.make_async_remote_copy(
            src_ref=deeps.at[to], dst_ref=deeps.at[NX + source],
            send_sem=send_sem.at[CHUNKS, to], recv_sem=recv_sem.at[CHUNKS, source],
            device_id={"tx": to}, device_id_type=MESH,
        )

    def rim_copy(to, source):
        return pltpu.make_async_remote_copy(
            src_ref=rim_low.at[to], dst_ref=rims.at[source],
            send_sem=rim_ssem.at[to], recv_sem=rim_rsem.at[source],
            device_id={"tx": to}, device_id_type=MESH,
        )

    def make(chunk, step):
        to = partner_of(tx, step)
        slot = jnp.where(step == NX - 1, NX + to, to)
        east = lax.rem(to + 1, NX)
        west = lax.rem(to + NX - 1, NX)
        at = pl.ds(pl.multiple_of(to * CI, CI), CI)
        low = jnp.zeros((BAND, LANES), f32)
        high = jnp.zeros((BAND, LANES), f32)
        if chunk == 0:
            deep = bottom[:, at]
            lane_from, row_from = packing(as_rows(deep), pltpu.roll)
            pack_lane[to] = lane_from
            pack_row[to] = row_from
            deep = deep.astype(f32)
            deeps[slot] = deep
            low = jnp.where(lanes == TIERS, pltpu.roll(deep[:, CI - LANES :], TIERS + 1, 1), low)
            high = jnp.where(lanes == 32 + TIERS, pltpu.roll(deep[:, :LANES], 32 + TIERS, 1), high)
        else:
            lane_from = pack_lane[to]
            row_from = pack_row[to]
        for tier in range(CUTS[chunk], CUTS[chunk + 1]):
            value = density(heat[tier, :, at], brine[tier, :, at], tier)
            boxes[slot, tier] = pack(as_rows(value), lane_from, row_from)
            low = jnp.where(lanes == tier, pltpu.roll(value[:, CI - LANES :], tier + 1, 1), low)
            high = jnp.where(lanes == 32 + tier, pltpu.roll(value[:, :LANES], 32 + tier, 1), high)
        if chunk == 0:
            rim_low[east] = low
            rim_high[west] = high
        else:
            rim_low[east] = rim_low[east] + low
            rim_high[west] = rim_high[west] + high

    def wait_loads(chunk):
        loads[1 + 2 * chunk].wait()
        loads[2 + 2 * chunk].wait()

    loads[0].wait()
    wait_loads(0)
    make(0, jnp.int32(0))
    neighbours = jnp.where(ty > 0, 1, 0) + jnp.where(ty < NY - 1, 1, 0)
    pl.semaphore_wait(barrier, NX - 1 + neighbours)

    def first_chunk(step, carry):
        make(0, step)
        to = partner_of(tx, step - 1)
        deep_copy(to, tx).start()
        box_copy(0, to, tx).start()
        return carry

    lax.fori_loop(1, NX, first_chunk, 0)
    for chunk in range(1, CHUNKS):
        wait_loads(chunk)

        def later_chunk(step, carry, chunk=chunk):
            make(chunk, step)
            return carry

        lax.fori_loop(0, NX, later_chunk, 0)

    def join(to, carry):
        rim_low[to] = rim_low[to] + rim_high[to]
        return carry

    lax.fori_loop(0, NX, join, 0)
    rims[tx] = rim_low[tx]

    def send_rim(step, carry):
        rim_copy(partner_of(tx, step), tx).start()
        return carry

    lax.fori_loop(0, NX - 1, send_rim, 0)
    for chunk in range(1, CHUNKS):

        def send_chunk(step, carry, chunk=chunk):
            box_copy(chunk, partner_of(tx, step), tx).start()
            return carry

        lax.fori_loop(0, NX - 1, send_chunk, 0)

    def arrive(chunk, source):
        @pl.when(source != tx)
        def _():
            if chunk == 0:
                deep_copy(source, source).wait_recv()
            box_copy(chunk, source, source).wait_recv()

        rows = pl.ds(pl.multiple_of(PAD + source * BAND, BAND), BAND)
        deep = deeps[NX + source]
        if chunk == 0:
            row_from, lane_from = unpacking(as_rows(deep))
            rows_back[source] = row_from
            pack_lane[source] = lane_from
            depth[rows] = deep
        else:
            row_from = rows_back[source]
            lane_from = pack_lane[source]
        for tier in range(CUTS[chunk], CUTS[chunk + 1]):
            value = as_block(unpack(boxes[NX + source, tier], row_from, lane_from))
            out[tier, rows] = jnp.where(deep > tier, value, 0.0)

    def row_copy(chunk, side, device):
        return pltpu.make_async_remote_copy(
            src_ref=rows_out.at[chunk, side], dst_ref=rows_in.at[chunk, 1 - side if device == "ty" else 1],
            send_sem=row_ssem.at[chunk, side], recv_sem=row_rsem.at[chunk, 1 - side if device == "ty" else 1],
            device_id={"ty": jnp.minimum(ty + 1, NY - 1) if side else jnp.maximum(ty - 1, 0)} if device == "ty" else {"tx": NX - 1 - tx},
            device_id_type=MESH,
        )

    def hand_on(chunk):
        @pl.when(ty > 0)
        def _():
            row_copy(chunk, 0, "ty").start()

        @pl.when(ty < NY - 1)
        def _():
            row_copy(chunk, 1, "ty").start()

        @pl.when(ty == NY - 1)
        def _():
            row_copy(chunk, 1, "tx").start()

    def rows_here(chunk):
        @pl.when(ty > 0)
        def _():
            row_copy(chunk, 0, "ty").wait_send()
            row_copy(chunk, 1, "ty").wait_recv()

        @pl.when(ty < NY - 1)
        def _():
            row_copy(chunk, 1, "ty").wait_send()
            row_copy(chunk, 0, "ty").wait_recv()

        @pl.when(ty == NY - 1)
        def _():
            row_copy(chunk, 1, "tx").wait()

        turn = 127 - lanes
        lower = rows_in[chunk, 0]
        upper = rows_in[chunk, 1]
        flipped = [jnp.take_along_axis(upper[:, LANES * v : LANES * v + LANES], turn, axis=1) for v in (3, 2, 1, 0)]
        upper = jnp.where(ty == NY - 1, jnp.concatenate(flipped, axis=1), upper)
        count = CUTS[chunk + 1] - CUTS[chunk]
        for number in range(count):
            out[CUTS[chunk] + number, PAD - 1 : PAD] = lower[number : number + 1]
            out[CUTS[chunk] + number, PAD + CJ : PAD + CJ + 1] = upper[number : number + 1]
        if chunk == 0:
            depth[PAD - 1 : PAD] = jnp.where(ty > 0, lower[count : count + 1], 0.0)
            depth[PAD + CJ : PAD + CJ + 1] = upper[count : count + 1]

    first_row = lax.broadcasted_iota(i32, (BAND, CI), 0) == 0
    last_row = lax.broadcasted_iota(i32, (BAND, CI), 0) == BAND - 1

    def around(ref, band, tier):
        here = ref[PAD + BAND * band : PAD + BAND * band + BAND]
        above = ref[PAD + BAND * band + BAND : PAD + BAND * band + 2 * BAND]
        below = ref[PAD + BAND * band - BAND : PAD + BAND * band]
        north = jnp.where(last_row, pltpu.roll(above, BAND - 1, 0), pltpu.roll(here, BAND - 1, 0))
        south = jnp.where(first_row, pltpu.roll(below, 1, 0), pltpu.roll(here, 1, 0))
        rim = rims[band]
        east = pltpu.roll(here, CI - 1, 1)
        east_rim = pltpu.roll(rim, (127 - 32 - tier + LANES) % LANES if isinstance(tier, int) else 127 - 32 - tier, 1)
        east = jnp.concatenate([east[:, : CI - LANES], jnp.where(lanes == 127, east_rim, east[:, CI - LANES :])], 1)
        west = pltpu.roll(here, 1, 1)
        west = jnp.concatenate([jnp.where(lanes == 0, pltpu.roll(rim, LANES - tier, 1), west[:, :LANES]), west[:, LANES:]], 1)
        return here, north, south, east, west

    def bounds(band):
        here, *others = around(depth, band, TIERS)
        for side, other in enumerate(others):
            least[side, BAND * band : BAND * band + BAND] = jnp.minimum(here, other)

    def laplace(chunk, bands):
        def one(tier, carry):
            level = tier.astype(f32)
            field = out.at[tier]
            for band in bands:
                here, *others = around(field, band, tier)
                total = None
                for side, other in enumerate(others):
                    term = jnp.where(least[side, BAND * band : BAND * band + BAND] > level, other - here, 0.0)
                    total = term if total is None else total + term
                lap[tier, BAND * band : BAND * band + BAND] = total
            return carry

        lax.fori_loop(CUTS[chunk], CUTS[chunk + 1], one, 0)

    inner = list(range(1, NX - 1))
    for chunk in range(CHUNKS):
        arrive(chunk, 0)
        arrive(chunk, NX - 1)
        count = CUTS[chunk + 1] - CUTS[chunk]
        for number in range(count):
            tier = CUTS[chunk] + number
            rows_out[chunk, 0, number : number + 1] = out[tier, PAD : PAD + 1]
            rows_out[chunk, 1, number : number + 1] = out[tier, PAD + CJ - 1 : PAD + CJ]
        if chunk == 0:
            rows_out[chunk, 0, count : count + 1] = depth[PAD : PAD + 1]
            rows_out[chunk, 1, count : count + 1] = depth[PAD + CJ - 1 : PAD + CJ]
        arrive(chunk, 1)
        hand_on(chunk)

        def rest(source, carry, chunk=chunk):
            arrive(chunk, source)
            return carry

        lax.fori_loop(2, NX - 1, rest, 0)
        if chunk == 0:

            def rim_in(source, carry):
                @pl.when(source != tx)
                def _():
                    rim_copy(source, source).wait_recv()

                return carry

            lax.fori_loop(0, NX, rim_in, 0)
            for band in inner:
                bounds(band)
        laplace(chunk, inner)
        rows_here(chunk)
        if chunk == 0:
            bounds(0)
            bounds(NX - 1)
        laplace(chunk, (0, NX - 1))

    def sent(to, carry):
        @pl.when(to != tx)
        def _():
            deep_copy(to, tx).wait_send()
            rim_copy(to, tx).wait_send()
            for chunk in range(CHUNKS):
                box_copy(chunk, to, tx).wait_send()

        return carry

    lax.fori_loop(0, NX, sent, 0)


def write_out(field, lap, field_out, lap_out, sem):
    copies = []
    for part in range(4):
        at = pl.ds(part * TIERS // 4, TIERS // 4)
        copies.append(pltpu.make_async_copy(field.at[at, PAD : PAD + CJ], field_out.at[at], sem.at[2 * part]))
        copies.append(pltpu.make_async_copy(lap.at[at], lap_out.at[at], sem.at[2 * part + 1]))
    for copy in copies:
        copy.start()
    for copy in copies:
        copy.wait()


def on_device(warmth, salt, tally):
    hbm = pl.BlockSpec(memory_space=pltpu.HBM)
    vmem = pl.BlockSpec(memory_space=pltpu.VMEM)
    field, lap = pl.pallas_call(
        exchange,
        out_shape=(pltpu.VMEM((TIERS, CJ + 2 * PAD, CI), f32), pltpu.VMEM((TIERS, CJ, CI), f32)),
        in_specs=[hbm] * 3,
        out_specs=(vmem,) * 2,
        scratch_shapes=[
            pltpu.VMEM((TIERS, BAND, COLS), f32),
            pltpu.VMEM((TIERS, BAND, COLS), f32),
            pltpu.VMEM((BAND, COLS), i32),
            pltpu.VMEM((2 * NX, TIERS, KEPT, LANES), f32),
            pltpu.VMEM((2 * NX, BAND, CI), f32),
            pltpu.VMEM((CJ + 2 * PAD, CI), f32),
            pltpu.VMEM((4, CJ, CI), f32),
            pltpu.VMEM((NX, ROWS, LANES), i32),
            pltpu.VMEM((NX, KEPT, LANES), i32),
            pltpu.VMEM((NX, ROWS, LANES), i32),
            pltpu.VMEM((NX, BAND, LANES), f32),
            pltpu.VMEM((NX, BAND, LANES), f32),
            pltpu.VMEM((NX, BAND, LANES), f32),
            pltpu.VMEM((CHUNKS, 2, BAND, CI), f32),
            pltpu.VMEM((CHUNKS, 2, BAND, CI), f32),
            pltpu.SemaphoreType.DMA((2 * CHUNKS + 1,)),
            pltpu.SemaphoreType.DMA((CHUNKS + 1, NX)),
            pltpu.SemaphoreType.DMA((CHUNKS + 1, NX)),
            pltpu.SemaphoreType.DMA((NX,)),
            pltpu.SemaphoreType.DMA((NX,)),
            pltpu.SemaphoreType.DMA((CHUNKS, 2)),
            pltpu.SemaphoreType.DMA((CHUNKS, 2)),
        ],
        compiler_params=pltpu.CompilerParams(collective_id=0, has_side_effects=True, vmem_limit_bytes=40 * 2**20),
        name="exchange",
    )(warmth, salt, tally)
    return pl.pallas_call(
        write_out,
        out_shape=(jax.ShapeDtypeStruct((TIERS, CJ, CI), f32),) * 2,
        in_specs=[pl.BlockSpec(memory_space=pl.ANY)] * 2,
        out_specs=(hbm,) * 2,
        scratch_shapes=[pltpu.SemaphoreType.DMA((8,))],
        compiler_params=pltpu.CompilerParams(vmem_limit_bytes=16 * 2**20),
        name="write_out",
    )(field, lap)


def solution(mesh):
    placed = (P(None, ("ty", "tx"), None), P(None, ("ty", "tx"), None), P(("ty", "tx"), None))
    return jax.shard_map(
        on_device,
        mesh=mesh,
        in_specs=placed,
        out_specs=(P(None, "ty", "tx"), P(None, "ty", "tx")),
        check_vma=False,
    )
```

```python
import jax
import jax.numpy as jnp
from jax import lax
from jax.experimental import pallas as pl
from jax.experimental.pallas import tpu as pltpu
from jax.sharding import PartitionSpec as P

therm_coef = 0.1655
haline_coef = 0.76554
cabbel_coef = 0.05952
haline_second = 0.00054914
thermo_press = 0.0001497
haline_press = 1.109e-05
cross_coef = 0.0024341

MESH = pl.DeviceIdType.MESH
TIERS = 16
BAND = 8
CJ = 128
CI = 512
NX = 16
NY = 8
COLS = NX * CI
LANES = 128
ROWS = BAND * CI // LANES
KEPT = 24
SPARE = (ROWS - KEPT) * LANES
CUTS = (0, 4, 8, 12, 16)
CHUNKS = len(CUTS) - 1
PAD = BAND
FAR = ((2, 2), (2, 1), (2, 3), (1, 2), (3, 2), (1, 1), (3, 3), (1, 3), (3, 1), (2, 0), (0, 2), (1, 0), (3, 0), (0, 1), (0, 3), (0, 0))
f32 = jnp.float32
i32 = jnp.int32


def density(warmth, salt, tier):
    depth = 5.0 + 10.0 * tier
    a = warmth - 10.0
    b = salt - 35.0
    heat = (-therm_coef * (1.0 + thermo_press * depth)) - (0.5 * therm_coef * cabbel_coef) * a - cross_coef * b
    salty = (haline_coef * (1.0 - haline_press * depth)) - (0.5 * haline_coef * haline_second) * b
    return heat * a + salty * b


def partner_of(tx, step):
    dy = jnp.int32(0)
    dz = jnp.int32(0)
    for number, (far_y, far_z) in enumerate(FAR):
        dy = jnp.where(step == number, far_y, dy)
        dz = jnp.where(step == number, far_z, dz)
    return ((tx // 4 + dy) & 3) * 4 + ((tx + dz) & 3)


def as_rows(block):
    return jnp.concatenate([block[:, LANES * v : LANES * v + LANES] for v in range(CI // LANES)], axis=0)


def as_block(rows):
    return jnp.concatenate([rows[BAND * v : BAND * v + BAND] for v in range(CI // LANES)], axis=1)


def land_counts(land):
    one = lax.broadcasted_iota(i32, (LANES, 2 * LANES), 0)
    two = lax.broadcasted_iota(i32, (LANES, 2 * LANES), 1)
    ahead = jnp.where(jnp.logical_or(two >= LANES, one < two), 1.0, 0.0).astype(jnp.bfloat16)
    both = jnp.dot(land.astype(jnp.bfloat16), ahead, preferred_element_type=f32)
    one = lax.broadcasted_iota(i32, (ROWS, ROWS), 0)
    two = lax.broadcasted_iota(i32, (ROWS, ROWS), 1)
    above = jnp.where(two < one, 1.0, 0.0).astype(jnp.bfloat16)
    start = jnp.dot(above, both[:, LANES:].astype(jnp.bfloat16), preferred_element_type=f32)
    cell = jnp.minimum(start + both[:, :LANES], float(SPARE))
    return jnp.minimum(start, float(SPARE)).astype(i32), cell.astype(i32)


def squeeze(state, bits, axis, roll):
    size = state.shape[axis]
    for bit in range(bits):
        flag = 256 << bit
        ahead = roll(state, size - (1 << bit), axis)
        stay = jnp.where((state & flag) != 0, 0, state)
        state = jnp.where((ahead & flag) != 0, ahead, stay)
    return state


def packing(tally, roll):
    start, cell = land_counts(jnp.where(tally > 0, 0.0, 1.0))
    lane = lax.broadcasted_iota(i32, (ROWS, LANES), 1)
    row = lax.broadcasted_iota(i32, (ROWS, LANES), 0)
    state = jnp.where(tally > 0, ((cell - start) << 8) | 128 | lane, 0)
    state = squeeze(state, 7, 1, roll) & 255
    state = jnp.take_along_axis(state, (lane + start) & 127, axis=1)
    back = (start + lane) >> 7
    rows = jnp.where(state >= 128, (back << 8) | row, 0)
    rows = squeeze(rows, 4, 0, roll) & 31
    return state & 127, rows[:KEPT]


def unpacking(tally):
    start, cell = land_counts(jnp.where(tally > 0, 0.0, 1.0))
    lane = lax.broadcasted_iota(i32, (ROWS, LANES), 1)
    row = lax.broadcasted_iota(i32, (ROWS, LANES), 0)
    return row - ((start + lane) >> 7), (lane - cell) & 127


def pack(rows, lane_from, row_from):
    moved = jnp.take_along_axis(rows, lane_from, axis=1)
    parts = []
    for w in range(KEPT // BAND):
        at = row_from[BAND * w : BAND * w + BAND]
        low = jnp.take_along_axis(moved[BAND * w : BAND * w + BAND], at & 7, axis=0)
        high = jnp.take_along_axis(moved[BAND * w + BAND : BAND * w + 2 * BAND], at & 7, axis=0)
        parts.append(jnp.where(at >= BAND * (w + 1), high, low))
    return jnp.concatenate(parts, axis=0)


def unpack(kept, row_from, lane_from):
    parts = []
    for v in range(ROWS // BAND):
        at = row_from[BAND * v : BAND * v + BAND]
        low = None if v == 0 else jnp.take_along_axis(kept[BAND * v - BAND : BAND * v], at & 7, axis=0)
        high = None if v == KEPT // BAND else jnp.take_along_axis(kept[BAND * v : BAND * v + BAND], at & 7, axis=0)
        if low is None or high is None:
            parts.append(high if low is None else low)
        else:
            parts.append(jnp.where(at >= BAND * v, high, low))
    return jnp.take_along_axis(jnp.concatenate(parts, axis=0), lane_from, axis=1)


def exchange(
    warmth, salt, tally, out, lap,
    heat, brine, bottom, boxes, deeps, depth, least, pack_lane, pack_row, rows_back, rim_low, rim_high, rims, rows_out, rows_in,
    in_sem, send_sem, recv_sem, rim_ssem, rim_rsem, row_ssem, row_rsem,
):
    ty = lax.axis_index("ty")
    tx = lax.axis_index("tx")
    barrier = pltpu.get_barrier_semaphore()
    loads = [pltpu.make_async_copy(tally, bottom, in_sem.at[2 * CHUNKS])]
    for chunk in range(CHUNKS):
        part = pl.ds(CUTS[chunk], CUTS[chunk + 1] - CUTS[chunk])
        loads.append(pltpu.make_async_copy(warmth.at[part], heat.at[part], in_sem.at[2 * chunk]))
        loads.append(pltpu.make_async_copy(salt.at[part], brine.at[part], in_sem.at[2 * chunk + 1]))
    for load in loads:
        load.start()
    for step in range(1, NX):
        pl.semaphore_signal(barrier, inc=1, device_id={"tx": lax.rem(tx + step, NX)}, device_id_type=MESH)

    @pl.when(ty > 0)
    def _():
        pl.semaphore_signal(barrier, inc=1, device_id={"ty": ty - 1}, device_id_type=MESH)

    @pl.when(ty < NY - 1)
    def _():
        pl.semaphore_signal(barrier, inc=1, device_id={"ty": ty + 1}, device_id_type=MESH)

    lanes = lax.broadcasted_iota(i32, (BAND, LANES), 1)

    def levels(chunk):
        return pl.ds(CUTS[chunk], CUTS[chunk + 1] - CUTS[chunk])

    def box_copy(chunk, to, source):
        return pltpu.make_async_remote_copy(
            src_ref=boxes.at[to, levels(chunk)], dst_ref=boxes.at[NX + source, levels(chunk)],
            send_sem=send_sem.at[chunk, to], recv_sem=recv_sem.at[chunk, source],
            device_id={"tx": to}, device_id_type=MESH,
        )

    def deep_copy(to, source):
        return pltpu.make_async_remote_copy(
            src_ref=deeps.at[to], dst_ref=deeps.at[NX + source],
            send_sem=send_sem.at[CHUNKS, to], recv_sem=recv_sem.at[CHUNKS, source],
            device_id={"tx": to}, device_id_type=MESH,
        )

    def rim_copy(to, source):
        return pltpu.make_async_remote_copy(
            src_ref=rim_low.at[to], dst_ref=rims.at[source],
            send_sem=rim_ssem.at[to], recv_sem=rim_rsem.at[source],
            device_id={"tx": to}, device_id_type=MESH,
        )

    def make(chunk, step):
        to = partner_of(tx, step)
        slot = jnp.where(step == NX - 1, NX + to, to)
        east = lax.rem(to + 1, NX)
        west = lax.rem(to + NX - 1, NX)
        at = pl.ds(pl.multiple_of(to * CI, CI), CI)
        low = jnp.zeros((BAND, LANES), f32)
        high = jnp.zeros((BAND, LANES), f32)
        if chunk == 0:
            deep = bottom[:, at]
            lane_from, row_from = packing(as_rows(deep), pltpu.roll)
            pack_lane[to] = lane_from
            pack_row[to] = row_from
            deep = deep.astype(f32)
            deeps[slot] = deep
            low = jnp.where(lanes == TIERS, pltpu.roll(deep[:, CI - LANES :], TIERS + 1, 1), low)
            high = jnp.where(lanes == 32 + TIERS, pltpu.roll(deep[:, :LANES], 32 + TIERS, 1), high)
        else:
            lane_from = pack_lane[to]
            row_from = pack_row[to]
        for tier in range(CUTS[chunk], CUTS[chunk + 1]):
            value = density(heat[tier, :, at], brine[tier, :, at], tier)
            boxes[slot, tier] = pack(as_rows(value), lane_from, row_from)
            low = jnp.where(lanes == tier, pltpu.roll(value[:, CI - LANES :], tier + 1, 1), low)
            high = jnp.where(lanes == 32 + tier, pltpu.roll(value[:, :LANES], 32 + tier, 1), high)
        if chunk == 0:
            rim_low[east] = low
            rim_high[west] = high
        else:
            rim_low[east] = rim_low[east] + low
            rim_high[west] = rim_high[west] + high

    def wait_loads(chunk):
        loads[1 + 2 * chunk].wait()
        loads[2 + 2 * chunk].wait()

    loads[0].wait()
    wait_loads(0)
    make(0, jnp.int32(0))
    neighbours = jnp.where(ty > 0, 1, 0) + jnp.where(ty < NY - 1, 1, 0)
    pl.semaphore_wait(barrier, NX - 1 + neighbours)

    def first_chunk(step, carry):
        make(0, step)
        to = partner_of(tx, step - 1)
        deep_copy(to, tx).start()
        box_copy(0, to, tx).start()
        return carry

    lax.fori_loop(1, NX, first_chunk, 0)
    for chunk in range(1, CHUNKS):
        wait_loads(chunk)

        def later_chunk(step, carry, chunk=chunk):
            make(chunk, step)
            return carry

        lax.fori_loop(0, NX, later_chunk, 0)

    def join(to, carry):
        rim_low[to] = rim_low[to] + rim_high[to]
        return carry

    lax.fori_loop(0, NX, join, 0)
    rims[tx] = rim_low[tx]

    partners = [((tx // 4 + dy) & 3) * 4 + ((tx + dz) & 3) for dy, dz in FAR[:-1]]
    for to in partners:
        rim_copy(to, tx).start()
    for chunk in range(1, CHUNKS):
        for to in partners:
            box_copy(chunk, to, tx).start()

    def arrive(chunk, source):
        @pl.when(source != tx)
        def _():
            if chunk == 0:
                deep_copy(source, source).wait_recv()
            box_copy(chunk, source, source).wait_recv()

        rows = pl.ds(pl.multiple_of(PAD + source * BAND, BAND), BAND)
        deep = deeps[NX + source]
        if chunk == 0:
            row_from, lane_from = unpacking(as_rows(deep))
            rows_back[source] = row_from
            pack_lane[source] = lane_from
            depth[rows] = deep
        else:
            row_from = rows_back[source]
            lane_from = pack_lane[source]
        for tier in range(CUTS[chunk], CUTS[chunk + 1]):
            value = as_block(unpack(boxes[NX + source, tier], row_from, lane_from))
            out[tier, rows] = jnp.where(deep > tier, value, 0.0)

    def row_copy(chunk, side, device):
        return pltpu.make_async_remote_copy(
            src_ref=rows_out.at[chunk, side], dst_ref=rows_in.at[chunk, 1 - side if device == "ty" else 1],
            send_sem=row_ssem.at[chunk, side], recv_sem=row_rsem.at[chunk, 1 - side if device == "ty" else 1],
            device_id={"ty": jnp.minimum(ty + 1, NY - 1) if side else jnp.maximum(ty - 1, 0)} if device == "ty" else {"tx": NX - 1 - tx},
            device_id_type=MESH,
        )

    def hand_on(chunk):
        @pl.when(ty > 0)
        def _():
            row_copy(chunk, 0, "ty").start()

        @pl.when(ty < NY - 1)
        def _():
            row_copy(chunk, 1, "ty").start()

        @pl.when(ty == NY - 1)
        def _():
            row_copy(chunk, 1, "tx").start()

    def rows_here(chunk):
        @pl.when(ty > 0)
        def _():
            row_copy(chunk, 0, "ty").wait_send()
            row_copy(chunk, 1, "ty").wait_recv()

        @pl.when(ty < NY - 1)
        def _():
            row_copy(chunk, 1, "ty").wait_send()
            row_copy(chunk, 0, "ty").wait_recv()

        @pl.when(ty == NY - 1)
        def _():
            row_copy(chunk, 1, "tx").wait()

        turn = 127 - lanes
        lower = rows_in[chunk, 0]
        upper = rows_in[chunk, 1]
        flipped = [jnp.take_along_axis(upper[:, LANES * v : LANES * v + LANES], turn, axis=1) for v in (3, 2, 1, 0)]
        upper = jnp.where(ty == NY - 1, jnp.concatenate(flipped, axis=1), upper)
        count = CUTS[chunk + 1] - CUTS[chunk]
        for number in range(count):
            out[CUTS[chunk] + number, PAD - 1 : PAD] = lower[number : number + 1]
            out[CUTS[chunk] + number, PAD + CJ : PAD + CJ + 1] = upper[number : number + 1]
        if chunk == 0:
            depth[PAD - 1 : PAD] = jnp.where(ty > 0, lower[count : count + 1], 0.0)
            depth[PAD + CJ : PAD + CJ + 1] = upper[count : count + 1]

    first_row = lax.broadcasted_iota(i32, (BAND, CI), 0) == 0
    last_row = lax.broadcasted_iota(i32, (BAND, CI), 0) == BAND - 1

    def around(ref, band, tier):
        here = ref[PAD + BAND * band : PAD + BAND * band + BAND]
        above = ref[PAD + BAND * band + BAND : PAD + BAND * band + 2 * BAND]
        below = ref[PAD + BAND * band - BAND : PAD + BAND * band]
        north = jnp.where(last_row, pltpu.roll(above, BAND - 1, 0), pltpu.roll(here, BAND - 1, 0))
        south = jnp.where(first_row, pltpu.roll(below, 1, 0), pltpu.roll(here, 1, 0))
        rim = rims[band]
        east = pltpu.roll(here, CI - 1, 1)
        east_rim = pltpu.roll(rim, (127 - 32 - tier + LANES) % LANES if isinstance(tier, int) else 127 - 32 - tier, 1)
        east = jnp.concatenate([east[:, : CI - LANES], jnp.where(lanes == 127, east_rim, east[:, CI - LANES :])], 1)
        west = pltpu.roll(here, 1, 1)
        west = jnp.concatenate([jnp.where(lanes == 0, pltpu.roll(rim, LANES - tier, 1), west[:, :LANES]), west[:, LANES:]], 1)
        return here, north, south, east, west

    def bounds(band):
        here, *others = around(depth, band, TIERS)
        for side, other in enumerate(others):
            least[side, BAND * band : BAND * band + BAND] = jnp.minimum(here, other)

    def laplace(chunk, bands, stop=None):
        def one(tier, carry):
            level = tier.astype(f32)
            field = out.at[tier]
            for band in bands:
                here, *others = around(field, band, tier)
                total = None
                for side, other in enumerate(others):
                    term = jnp.where(least[side, BAND * band : BAND * band + BAND] > level, other - here, 0.0)
                    total = term if total is None else total + term
                lap[tier, BAND * band : BAND * band + BAND] = total
            return carry

        lax.fori_loop(CUTS[chunk], CUTS[chunk + 1] if stop is None else stop, one, 0)

    inner = list(range(1, NX - 1))
    for chunk in range(CHUNKS):
        arrive(chunk, 0)
        arrive(chunk, NX - 1)
        count = CUTS[chunk + 1] - CUTS[chunk]
        for number in range(count):
            tier = CUTS[chunk] + number
            rows_out[chunk, 0, number : number + 1] = out[tier, PAD : PAD + 1]
            rows_out[chunk, 1, number : number + 1] = out[tier, PAD + CJ - 1 : PAD + CJ]
        if chunk == 0:
            rows_out[chunk, 0, count : count + 1] = depth[PAD : PAD + 1]
            rows_out[chunk, 1, count : count + 1] = depth[PAD + CJ - 1 : PAD + CJ]
        arrive(chunk, 1)
        hand_on(chunk)

        def rest(source, carry, chunk=chunk):
            arrive(chunk, source)
            return carry

        lax.fori_loop(2, NX - 1, rest, 0)
        if chunk == 0:

            def rim_in(source, carry):
                @pl.when(source != tx)
                def _():
                    rim_copy(source, source).wait_recv()

                return carry

            lax.fori_loop(0, NX, rim_in, 0)
            for band in inner:
                bounds(band)
        laplace(chunk, inner)

    for chunk in range(CHUNKS):
        rows_here(chunk)
    bounds(0)
    bounds(NX - 1)
    laplace(0, (0, NX - 1), TIERS)

    def sent(to, carry):
        @pl.when(to != tx)
        def _():
            deep_copy(to, tx).wait_send()
            rim_copy(to, tx).wait_send()
            for chunk in range(CHUNKS):
                box_copy(chunk, to, tx).wait_send()

        return carry

    lax.fori_loop(0, NX, sent, 0)


def write_out(field, lap, field_out, lap_out, sem):
    copies = []
    for part in range(4):
        at = pl.ds(part * TIERS // 4, TIERS // 4)
        copies.append(pltpu.make_async_copy(field.at[at, PAD : PAD + CJ], field_out.at[at], sem.at[2 * part]))
        copies.append(pltpu.make_async_copy(lap.at[at], lap_out.at[at], sem.at[2 * part + 1]))
    for copy in copies:
        copy.start()
    for copy in copies:
        copy.wait()


def on_device(warmth, salt, tally):
    hbm = pl.BlockSpec(memory_space=pltpu.HBM)
    vmem = pl.BlockSpec(memory_space=pltpu.VMEM)
    field, lap = pl.pallas_call(
        exchange,
        out_shape=(pltpu.VMEM((TIERS, CJ + 2 * PAD, CI), f32), pltpu.VMEM((TIERS, CJ, CI), f32)),
        in_specs=[hbm] * 3,
        out_specs=(vmem,) * 2,
        scratch_shapes=[
            pltpu.VMEM((TIERS, BAND, COLS), f32),
            pltpu.VMEM((TIERS, BAND, COLS), f32),
            pltpu.VMEM((BAND, COLS), i32),
            pltpu.VMEM((2 * NX, TIERS, KEPT, LANES), f32),
            pltpu.VMEM((2 * NX, BAND, CI), f32),
            pltpu.VMEM((CJ + 2 * PAD, CI), f32),
            pltpu.VMEM((4, CJ, CI), f32),
            pltpu.VMEM((NX, ROWS, LANES), i32),
            pltpu.VMEM((NX, KEPT, LANES), i32),
            pltpu.VMEM((NX, ROWS, LANES), i32),
            pltpu.VMEM((NX, BAND, LANES), f32),
            pltpu.VMEM((NX, BAND, LANES), f32),
            pltpu.VMEM((NX, BAND, LANES), f32),
            pltpu.VMEM((CHUNKS, 2, BAND, CI), f32),
            pltpu.VMEM((CHUNKS, 2, BAND, CI), f32),
            pltpu.SemaphoreType.DMA((2 * CHUNKS + 1,)),
            pltpu.SemaphoreType.DMA((CHUNKS + 1, NX)),
            pltpu.SemaphoreType.DMA((CHUNKS + 1, NX)),
            pltpu.SemaphoreType.DMA((NX,)),
            pltpu.SemaphoreType.DMA((NX,)),
            pltpu.SemaphoreType.DMA((CHUNKS, 2)),
            pltpu.SemaphoreType.DMA((CHUNKS, 2)),
        ],
        compiler_params=pltpu.CompilerParams(collective_id=0, has_side_effects=True, vmem_limit_bytes=50 * 2**20),
        name="exchange",
    )(warmth, salt, tally)
    return pl.pallas_call(
        write_out,
        out_shape=(jax.ShapeDtypeStruct((TIERS, CJ, CI), f32),) * 2,
        in_specs=[pl.BlockSpec(memory_space=pl.ANY)] * 2,
        out_specs=(hbm,) * 2,
        scratch_shapes=[pltpu.SemaphoreType.DMA((8,))],
        compiler_params=pltpu.CompilerParams(vmem_limit_bytes=16 * 2**20),
        name="write_out",
    )(field, lap)


def solution(mesh):
    placed = (P(None, ("ty", "tx"), None), P(None, ("ty", "tx"), None), P(("ty", "tx"), None))
    return jax.shard_map(
        on_device,
        mesh=mesh,
        in_specs=placed,
        out_specs=(P(None, "ty", "tx"), P(None, "ty", "tx")),
        check_vma=False,
    )
```

```python
import jax
import jax.numpy as jnp
from jax import lax
from jax.experimental import pallas as pl
from jax.experimental.pallas import tpu as pltpu
from jax.sharding import PartitionSpec as P

therm_coef = 0.1655
haline_coef = 0.76554
cabbel_coef = 0.05952
haline_second = 0.00054914
thermo_press = 0.0001497
haline_press = 1.109e-05
cross_coef = 0.0024341

MESH = pl.DeviceIdType.MESH
TIERS = 16
BAND = 8
CJ = 128
CI = 512
NX = 16
NY = 8
COLS = NX * CI
LANES = 128
ROWS = BAND * CI // LANES
KEPT = 24
SPARE = (ROWS - KEPT) * LANES
CUTS = (0, 5, 10, 14, 16)
CHUNKS = len(CUTS) - 1
EARLY = CUTS[-2]
BOX = ROWS + TIERS * KEPT
INNER = range(1, NX - 1)
LAST = NX - 1
FAR = ((2, 2), (2, 1), (2, 3), (1, 2), (3, 2), (1, 1), (3, 3), (1, 3), (3, 1), (2, 0), (0, 2), (1, 0), (3, 0), (0, 1), (0, 3), (0, 0))
f32 = jnp.float32
i32 = jnp.int32


def density(warmth, salt, tier):
    depth = 5.0 + 10.0 * tier
    a = warmth - 10.0
    b = salt - 35.0
    heat = (-therm_coef * (1.0 + thermo_press * depth)) - (0.5 * therm_coef * cabbel_coef) * a - cross_coef * b
    salty = (haline_coef * (1.0 - haline_press * depth)) - (0.5 * haline_coef * haline_second) * b
    return heat * a + salty * b


def partner_of(tx, step):
    dy = jnp.int32(0)
    dz = jnp.int32(0)
    for number, (far_y, far_z) in enumerate(FAR):
        dy = jnp.where(step == number, far_y, dy)
        dz = jnp.where(step == number, far_z, dz)
    return ((tx // 4 + dy) & 3) * 4 + ((tx + dz) & 3)


def as_rows(block):
    return jnp.concatenate([block[:, LANES * v : LANES * v + LANES] for v in range(CI // LANES)], axis=0)


def as_block(rows):
    return jnp.concatenate([rows[BAND * v : BAND * v + BAND] for v in range(CI // LANES)], axis=1)


def land_counts(land):
    one = lax.broadcasted_iota(i32, (LANES, 2 * LANES), 0)
    two = lax.broadcasted_iota(i32, (LANES, 2 * LANES), 1)
    ahead = jnp.where(jnp.logical_or(two >= LANES, one < two), 1.0, 0.0).astype(jnp.bfloat16)
    both = jnp.dot(land.astype(jnp.bfloat16), ahead, preferred_element_type=f32)
    one = lax.broadcasted_iota(i32, (ROWS, ROWS), 0)
    two = lax.broadcasted_iota(i32, (ROWS, ROWS), 1)
    above = jnp.where(two < one, 1.0, 0.0).astype(jnp.bfloat16)
    start = jnp.dot(above, both[:, LANES:].astype(jnp.bfloat16), preferred_element_type=f32)
    cell = jnp.minimum(start + both[:, :LANES], float(SPARE))
    return jnp.minimum(start, float(SPARE)).astype(i32), cell.astype(i32)


def squeeze(state, bits, axis, roll):
    size = state.shape[axis]
    for bit in range(bits):
        flag = 256 << bit
        ahead = roll(state, size - (1 << bit), axis)
        stay = jnp.where((state & flag) != 0, 0, state)
        state = jnp.where((ahead & flag) != 0, ahead, stay)
    return state


def packing(tally, roll):
    start, cell = land_counts(jnp.where(tally > 0, 0.0, 1.0))
    lane = lax.broadcasted_iota(i32, (ROWS, LANES), 1)
    row = lax.broadcasted_iota(i32, (ROWS, LANES), 0)
    state = jnp.where(tally > 0, ((cell - start) << 8) | 128 | lane, 0)
    state = squeeze(state, 7, 1, roll) & 255
    state = jnp.take_along_axis(state, (lane + start) & 127, axis=1)
    back = (start + lane) >> 7
    rows = jnp.where(state >= 128, (back << 8) | row, 0)
    rows = squeeze(rows, 4, 0, roll) & 31
    return state & 127, rows[:KEPT]


def unpacking(tally):
    start, cell = land_counts(jnp.where(tally > 0, 0.0, 1.0))
    lane = lax.broadcasted_iota(i32, (ROWS, LANES), 1)
    row = lax.broadcasted_iota(i32, (ROWS, LANES), 0)
    return row - ((start + lane) >> 7), (lane - cell) & 127


def pack(rows, lane_from, row_from):
    moved = jnp.take_along_axis(rows, lane_from, axis=1)
    parts = []
    for w in range(KEPT // BAND):
        at = row_from[BAND * w : BAND * w + BAND]
        low = jnp.take_along_axis(moved[BAND * w : BAND * w + BAND], at & 7, axis=0)
        high = jnp.take_along_axis(moved[BAND * w + BAND : BAND * w + 2 * BAND], at & 7, axis=0)
        parts.append(jnp.where(at >= BAND * (w + 1), high, low))
    return jnp.concatenate(parts, axis=0)


def unpack(kept, row_from, lane_from):
    parts = []
    for v in range(ROWS // BAND):
        at = row_from[BAND * v : BAND * v + BAND]
        low = None if v == 0 else jnp.take_along_axis(kept[BAND * v - BAND : BAND * v], at & 7, axis=0)
        high = None if v == KEPT // BAND else jnp.take_along_axis(kept[BAND * v : BAND * v + BAND], at & 7, axis=0)
        if low is None or high is None:
            parts.append(high if low is None else low)
        else:
            parts.append(jnp.where(at >= BAND * v, high, low))
    return jnp.take_along_axis(jnp.concatenate(parts, axis=0), lane_from, axis=1)


def around(ref, band, tier, rims, above=None, below=None):
    lanes = lax.broadcasted_iota(i32, (BAND, LANES), 1)
    row = lax.broadcasted_iota(i32, (BAND, CI), 0)
    here = ref[BAND * band : BAND * band + BAND]
    if above is None:
        above = pltpu.roll(ref[BAND * band + BAND : BAND * band + 2 * BAND], BAND - 1, 0)
    if below is None:
        below = pltpu.roll(ref[BAND * band - BAND : BAND * band], 1, 0)
    north = jnp.where(row == BAND - 1, above, pltpu.roll(here, BAND - 1, 0))
    south = jnp.where(row == 0, below, pltpu.roll(here, 1, 0))
    rim = rims[band]
    east = pltpu.roll(here, CI - 1, 1)
    east_rim = pltpu.roll(rim, 127 - 32 - tier, 1)
    east = jnp.concatenate([east[:, : CI - LANES], jnp.where(lanes == 127, east_rim, east[:, CI - LANES :])], 1)
    west = pltpu.roll(here, 1, 1)
    west_rim = pltpu.roll(rim, LANES - tier, 1)
    west = jnp.concatenate([jnp.where(lanes == 0, west_rim, west[:, :LANES]), west[:, LANES:]], 1)
    return here, north, south, east, west


def divergence(cells, bounds, level):
    here, *others = cells
    total = None
    for bound, other in zip(bounds, others):
        term = jnp.where(bound > level, other - here, 0.0)
        total = term if total is None else total + term
    return total


def exchange(
    warmth, salt, tally, out, lap, depth, least, rims, edges,
    heat, brine, bottom, boxes, pack_lane, pack_row, lane_back, row_back, rim_low, rim_high, brink_out, brink_in, rows_out, rows_in,
    in_sem, send_sem, recv_sem, rim_ssem, rim_rsem, brink_ssem, brink_rsem, row_ssem, row_rsem,
):
    ty = lax.axis_index("ty")
    tx = lax.axis_index("tx")
    outer = jnp.logical_or(tx == 0, tx == LAST)
    barrier = pltpu.get_barrier_semaphore()
    loads = [pltpu.make_async_copy(tally, bottom, in_sem.at[2 * CHUNKS])]
    for chunk in range(CHUNKS):
        part = pl.ds(CUTS[chunk], CUTS[chunk + 1] - CUTS[chunk])
        loads.append(pltpu.make_async_copy(warmth.at[part], heat.at[part], in_sem.at[2 * chunk]))
        loads.append(pltpu.make_async_copy(salt.at[part], brine.at[part], in_sem.at[2 * chunk + 1]))
    for step in range(1, NX):
        pl.semaphore_signal(barrier, inc=1, device_id={"tx": (tx + step) & LAST}, device_id_type=MESH)

    @pl.when(ty > 0)
    def _():
        pl.semaphore_signal(barrier, inc=1, device_id={"ty": ty - 1}, device_id_type=MESH)

    @pl.when(ty < NY - 1)
    def _():
        pl.semaphore_signal(barrier, inc=1, device_id={"ty": ty + 1}, device_id_type=MESH)

    for load in loads:
        load.start()
    lanes = lax.broadcasted_iota(i32, (BAND, LANES), 1)
    partners = [((tx // 4 + dy) & 3) * 4 + ((tx + dz) & 3) for dy, dz in FAR[:-1]]

    def box_copy(chunk, to, source):
        low = 0 if chunk == 0 else ROWS + KEPT * CUTS[chunk]
        part = pl.ds(low, ROWS + KEPT * CUTS[chunk + 1] - low)
        return pltpu.make_async_remote_copy(
            src_ref=boxes.at[to, part], dst_ref=boxes.at[NX + source, part],
            send_sem=send_sem.at[chunk, to], recv_sem=recv_sem.at[chunk, source],
            device_id={"tx": to}, device_id_type=MESH,
        )

    def rim_copy(to, source):
        return pltpu.make_async_remote_copy(
            src_ref=rim_low.at[to], dst_ref=rims.at[source],
            send_sem=rim_ssem.at[to], recv_sem=rim_rsem.at[source],
            device_id={"tx": to}, device_id_type=MESH,
        )

    def brink_copy(to, source):
        side = jnp.where(source == 0, 0, 1)
        return pltpu.make_async_remote_copy(
            src_ref=brink_out.at[to], dst_ref=brink_in.at[side],
            send_sem=brink_ssem.at[to], recv_sem=brink_rsem.at[side],
            device_id={"tx": to}, device_id_type=MESH,
        )

    def make(first, last, step):
        to = partner_of(tx, step)
        slot = jnp.where(step == LAST, NX + to, to)
        east = (to + 1) & LAST
        west = (to + LAST) & LAST
        at = pl.ds(pl.multiple_of(to * CI, CI), CI)
        low = jnp.zeros((BAND, LANES), f32)
        high = jnp.zeros((BAND, LANES), f32)
        if first == 0:
            deep = bottom[:, at]
            lane_from, row_from = packing(as_rows(deep), pltpu.roll)
            pack_lane[to] = lane_from
            pack_row[to] = row_from
            deep = deep.astype(f32)
            boxes[slot, :ROWS] = as_rows(deep)
            low = jnp.where(lanes == TIERS, pltpu.roll(deep[:, CI - LANES :], TIERS + 1, 1), low)
            high = jnp.where(lanes == 32 + TIERS, pltpu.roll(deep[:, :LANES], 32 + TIERS, 1), high)
        else:
            lane_from = pack_lane[to]
            row_from = pack_row[to]
        for tier in range(first, last):
            value = density(heat[tier, :, at], brine[tier, :, at], tier)
            boxes[slot, ROWS + KEPT * tier : ROWS + KEPT * tier + KEPT] = pack(as_rows(value), lane_from, row_from)
            low = jnp.where(lanes == tier, pltpu.roll(value[:, CI - LANES :], tier + 1, 1), low)
            high = jnp.where(lanes == 32 + tier, pltpu.roll(value[:, :LANES], 32 + tier, 1), high)
            if tier >= EARLY:
                brink = jnp.where(tx == 0, value[:1], value[BAND - 1 :])
                for v in range(CI // LANES):
                    place = (tier - EARLY) * (CI // LANES) + v
                    brink_out[to, place : place + 1] = brink[:, LANES * v : LANES * v + LANES]
        if first == 0:
            rim_low[east] = low
            rim_high[west] = high
        else:
            rim_low[east] = rim_low[east] + low
            rim_high[west] = rim_high[west] + high

    def wait_loads(chunk):
        loads[1 + 2 * chunk].wait()
        loads[2 + 2 * chunk].wait()

    def make_only(first, last):
        def one(step, carry):
            make(first, last, step)
            return carry

        return one

    def make_and_send(chunk):
        def one(step, carry):
            make(CUTS[chunk], CUTS[chunk + 1], step)

            @pl.when(step > 0)
            def _():
                box_copy(chunk, partner_of(tx, step - 1), tx).start()

            return carry

        return one

    loads[0].wait()
    wait_loads(0)
    lax.fori_loop(0, 3, make_only(CUTS[0], CUTS[1]), 0)
    neighbours = jnp.where(ty > 0, 1, 0) + jnp.where(ty < NY - 1, 1, 0)
    pl.semaphore_wait(barrier, NX - 1 + neighbours)
    for to in partners[:2]:
        box_copy(0, to, tx).start()
    lax.fori_loop(3, NX, make_and_send(0), 0)
    wait_loads(1)
    lax.fori_loop(0, NX, make_and_send(1), 0)
    wait_loads(2)
    wait_loads(3)
    lax.fori_loop(0, NX, make_only(CUTS[2], CUTS[4]), 0)

    def join(to, carry):
        rim_low[to] = rim_low[to] + rim_high[to]
        return carry

    lax.fori_loop(0, NX, join, 0)
    rims[tx] = rim_low[tx]

    @pl.when(outer)
    def _():
        brink_in[jnp.where(tx == 0, 0, 1)] = brink_out[tx]
        for to in partners:
            brink_copy(to, tx).start()

    for to in partners:
        rim_copy(to, tx).start()
    for chunk in (2, 3):
        for to in partners:
            box_copy(chunk, to, tx).start()

    def arrive(chunk, source):
        @pl.when(source != tx)
        def _():
            box_copy(chunk, source, source).wait_recv()

        rows = pl.ds(pl.multiple_of(source * BAND, BAND), BAND)
        deep = boxes[NX + source, :ROWS]
        if chunk == 0:
            row_from, lane_from = unpacking(deep)
            row_back[source] = row_from
            lane_back[source] = lane_from
            deep = as_block(deep)
            depth[rows] = deep
        else:
            row_from = row_back[source]
            lane_from = lane_back[source]
            deep = as_block(deep)
        for tier in range(CUTS[chunk], CUTS[chunk + 1]):
            kept = boxes[NX + source, ROWS + KEPT * tier : ROWS + KEPT * tier + KEPT]
            out[tier, rows] = jnp.where(deep > tier, as_block(unpack(kept, row_from, lane_from)), 0.0)

    def arrive_all(chunk, first=0, last=NX):
        def one(source, carry):
            arrive(chunk, source)
            return carry

        lax.fori_loop(first, last, one, 0)

    def laplace(chunk):
        def one(tier, carry):
            for band in INNER:
                rows = slice(BAND * band, BAND * band + BAND)
                bounds = [least[side, rows] for side in range(4)]
                lap[tier, rows] = divergence(around(out.at[tier], band, tier, rims), bounds, tier.astype(f32))
            return carry

        lax.fori_loop(CUTS[chunk], CUTS[chunk + 1], one, 0)

    arrive_all(0)
    arrive_all(1)

    def rim_in(source, carry):
        @pl.when(source != tx)
        def _():
            rim_copy(source, source).wait_recv()

        return carry

    lax.fori_loop(0, NX, rim_in, 0)
    for band in INNER:
        here, *others = around(depth, band, TIERS, rims)
        for side, other in enumerate(others):
            least[side, BAND * band : BAND * band + BAND] = jnp.minimum(here, other)
    laplace(0)
    laplace(1)

    arrive(2, 0)
    arrive(2, LAST)
    for side, at in ((0, 0), (1, CJ - 1)):
        @pl.when(tx != (LAST if side else 0))
        def _():
            brink_copy(LAST if side else 0, LAST if side else 0).wait_recv()

        for tier in range(EARLY):
            rows_out[side, tier : tier + 1] = out[tier, at : at + 1]
        rows_out[side, TIERS : TIERS + 1] = depth[at : at + 1]
        for place in range((TIERS - EARLY) * CI // LANES):
            tier, v = EARLY + place // (CI // LANES), place % (CI // LANES)
            rows_out[side, tier : tier + 1, LANES * v : LANES * v + LANES] = brink_in[side, place : place + 1]

    arrive(2, 1)

    def row_copy(side, along):
        place = 1 - side if along == "ty" else 1
        if along == "ty":
            device = {"ty": jnp.minimum(ty + 1, NY - 1) if side else jnp.maximum(ty - 1, 0)}
        else:
            device = {"tx": LAST - tx}
        return pltpu.make_async_remote_copy(
            src_ref=rows_out.at[side], dst_ref=rows_in.at[place], send_sem=row_ssem.at[side], recv_sem=row_rsem.at[place],
            device_id=device, device_id_type=MESH,
        )

    @pl.when(ty > 0)
    def _():
        row_copy(0, "ty").start()

    @pl.when(ty < NY - 1)
    def _():
        row_copy(1, "ty").start()

    @pl.when(ty == NY - 1)
    def _():
        row_copy(1, "tx").start()

    arrive_all(2, 2, LAST)
    laplace(2)
    arrive_all(3)

    @pl.when(ty > 0)
    def _():
        row_copy(0, "ty").wait_send()
        row_copy(1, "ty").wait_recv()

    @pl.when(ty < NY - 1)
    def _():
        row_copy(1, "ty").wait_send()
        row_copy(0, "ty").wait_recv()

    @pl.when(ty == NY - 1)
    def _():
        row_copy(1, "tx").wait()

    edges[0] = rows_in[0]
    edges[0, TIERS : TIERS + 1] = jnp.where(ty > 0, rows_in[0, TIERS : TIERS + 1], 0.0)
    turn = 127 - lax.broadcasted_iota(i32, (24, LANES), 1)
    upper = rows_in[1]
    flipped = [jnp.take_along_axis(upper[:, LANES * v : LANES * v + LANES], turn, axis=1) for v in (3, 2, 1, 0)]
    edges[1] = jnp.where(ty == NY - 1, jnp.concatenate(flipped, axis=1), upper)

    @pl.when(outer)
    def _():
        for to in partners:
            brink_copy(to, tx).wait_send()

    for to in partners:
        rim_copy(to, tx).wait_send()
        for chunk in range(CHUNKS):
            box_copy(chunk, to, tx).wait_send()


def finish(field, lap, depth, least, rims, edges, field_out, lap_out, ends, late, sem):
    middle = pl.ds(BAND, CJ - 2 * BAND)
    half = TIERS // 2
    copies = [pltpu.make_async_copy(field.at[pl.ds(half * n, half)], field_out.at[pl.ds(half * n, half)], sem.at[n]) for n in (0, 1)]
    copies.append(pltpu.make_async_copy(lap.at[pl.ds(0, EARLY), middle], lap_out.at[pl.ds(0, EARLY), middle], sem.at[2]))
    for copy in copies:
        copy.start()

    def outer(ref, tier, band):
        row = edges[1 if band else 0, tier : tier + 1]
        return around(ref, band, tier, rims, **{"above" if band else "below": row})

    for place, band in enumerate((0, LAST)):
        here, *others = outer(depth, TIERS, band)
        bounds = [jnp.minimum(here, other) for other in others]
        for tier in range(TIERS):
            ends[place, tier] = divergence(outer(field.at[tier], tier, band), bounds, tier)
        copies.append(pltpu.make_async_copy(ends.at[place], lap_out.at[:, pl.ds(BAND * band, BAND)], sem.at[3 + place]))
        copies[-1].start()
    for tier in range(EARLY, TIERS):
        for band in INNER:
            bounds = [least[side, BAND * band : BAND * band + BAND] for side in range(4)]
            late[tier - EARLY, BAND * (band - 1) : BAND * band] = divergence(around(field.at[tier], band, tier, rims), bounds, tier)
    copies.append(pltpu.make_async_copy(late, lap_out.at[pl.ds(EARLY, TIERS - EARLY), middle], sem.at[5]))
    copies[-1].start()
    for copy in copies:
        copy.wait()


def on_device(warmth, salt, tally):
    hbm = pl.BlockSpec(memory_space=pltpu.HBM)
    vmem = pl.BlockSpec(memory_space=pltpu.VMEM)
    held = pl.pallas_call(
        exchange,
        out_shape=(
            pltpu.VMEM((TIERS, CJ, CI), f32),
            pltpu.VMEM((TIERS, CJ, CI), f32),
            pltpu.VMEM((CJ, CI), f32),
            pltpu.VMEM((4, CJ, CI), f32),
            pltpu.VMEM((NX, BAND, LANES), f32),
            pltpu.VMEM((2, 24, CI), f32),
        ),
        in_specs=[hbm] * 3,
        out_specs=(vmem,) * 6,
        scratch_shapes=[
            pltpu.VMEM((TIERS, BAND, COLS), f32),
            pltpu.VMEM((TIERS, BAND, COLS), f32),
            pltpu.VMEM((BAND, COLS), i32),
            pltpu.VMEM((2 * NX, BOX, LANES), f32),
            pltpu.VMEM((NX, ROWS, LANES), i32),
            pltpu.VMEM((NX, KEPT, LANES), i32),
            pltpu.VMEM((NX, ROWS, LANES), i32),
            pltpu.VMEM((NX, ROWS, LANES), i32),
            pltpu.VMEM((NX, BAND, LANES), f32),
            pltpu.VMEM((NX, BAND, LANES), f32),
            pltpu.VMEM((NX, BAND, LANES), f32),
            pltpu.VMEM((2, BAND, LANES), f32),
            pltpu.VMEM((2, 24, CI), f32),
            pltpu.VMEM((2, 24, CI), f32),
            pltpu.SemaphoreType.DMA((2 * CHUNKS + 1,)),
            pltpu.SemaphoreType.DMA((CHUNKS, NX)),
            pltpu.SemaphoreType.DMA((CHUNKS, NX)),
            pltpu.SemaphoreType.DMA((NX,)),
            pltpu.SemaphoreType.DMA((NX,)),
            pltpu.SemaphoreType.DMA((NX,)),
            pltpu.SemaphoreType.DMA((2,)),
            pltpu.SemaphoreType.DMA((2,)),
            pltpu.SemaphoreType.DMA((2,)),
        ],
        compiler_params=pltpu.CompilerParams(collective_id=0, has_side_effects=True, vmem_limit_bytes=48 * 2**20),
        name="exchange",
    )(warmth, salt, tally)
    return pl.pallas_call(
        finish,
        out_shape=(jax.ShapeDtypeStruct((TIERS, CJ, CI), f32),) * 2,
        in_specs=[vmem] * 6,
        out_specs=(hbm,) * 2,
        scratch_shapes=[
            pltpu.VMEM((2, TIERS, BAND, CI), f32),
            pltpu.VMEM((TIERS - EARLY, CJ - 2 * BAND, CI), f32),
            pltpu.SemaphoreType.DMA((6,)),
        ],
        compiler_params=pltpu.CompilerParams(vmem_limit_bytes=16 * 2**20),
        name="finish",
    )(*held)


def solution(mesh):
    placed = (P(None, ("ty", "tx"), None), P(None, ("ty", "tx"), None), P(("ty", "tx"), None))
    return jax.shard_map(
        on_device,
        mesh=mesh,
        in_specs=placed,
        out_specs=(P(None, "ty", "tx"), P(None, "ty", "tx")),
        check_vma=False,
    )
```

```python
import jax
import jax.numpy as jnp
from jax import lax
from jax.experimental import pallas as pl
from jax.experimental.pallas import tpu as pltpu
from jax.sharding import PartitionSpec as P

therm_coef = 0.1655
haline_coef = 0.76554
cabbel_coef = 0.05952
haline_second = 0.00054914
thermo_press = 0.0001497
haline_press = 1.109e-05
cross_coef = 0.0024341

MESH = pl.DeviceIdType.MESH
TIERS = 16
BAND = 8
CJ = 128
CI = 512
NX = 16
NY = 8
COLS = NX * CI
LANES = 128
ROWS = BAND * CI // LANES
KEPT = 24
SPARE = (ROWS - KEPT) * LANES
CUTS = (0, 5, 10, 14, 16)
CHUNKS = len(CUTS) - 1
EARLY = CUTS[-2]
BOX = ROWS + TIERS * KEPT
INNER = range(1, NX - 1)
LAST = NX - 1
FAR = ((0, 2), (2, 2), (0, 1), (1, 1), (3, 3), (0, 3), (2, 1), (2, 3), (1, 2), (3, 2), (1, 3), (3, 1), (2, 0), (1, 0), (3, 0), (0, 0))
f32 = jnp.float32
i32 = jnp.int32


def density(warmth, salt, tier):
    depth = 5.0 + 10.0 * tier
    a = warmth - 10.0
    b = salt - 35.0
    heat = (-therm_coef * (1.0 + thermo_press * depth)) - (0.5 * therm_coef * cabbel_coef) * a - cross_coef * b
    salty = (haline_coef * (1.0 - haline_press * depth)) - (0.5 * haline_coef * haline_second) * b
    return heat * a + salty * b


def partner_of(tx, step):
    dy = jnp.int32(0)
    dz = jnp.int32(0)
    for number, (far_y, far_z) in enumerate(FAR):
        dy = jnp.where(step == number, far_y, dy)
        dz = jnp.where(step == number, far_z, dz)
    return ((tx // 4 + dy) & 3) * 4 + ((tx + dz) & 3)


def as_rows(block):
    return jnp.concatenate([block[:, LANES * v : LANES * v + LANES] for v in range(CI // LANES)], axis=0)


def as_block(rows):
    return jnp.concatenate([rows[BAND * v : BAND * v + BAND] for v in range(CI // LANES)], axis=1)


def land_counts(land):
    one = lax.broadcasted_iota(i32, (LANES, 2 * LANES), 0)
    two = lax.broadcasted_iota(i32, (LANES, 2 * LANES), 1)
    ahead = jnp.where(jnp.logical_or(two >= LANES, one < two), 1.0, 0.0).astype(jnp.bfloat16)
    both = jnp.dot(land.astype(jnp.bfloat16), ahead, preferred_element_type=f32)
    one = lax.broadcasted_iota(i32, (ROWS, ROWS), 0)
    two = lax.broadcasted_iota(i32, (ROWS, ROWS), 1)
    above = jnp.where(two < one, 1.0, 0.0).astype(jnp.bfloat16)
    start = jnp.dot(above, both[:, LANES:].astype(jnp.bfloat16), preferred_element_type=f32)
    cell = jnp.minimum(start + both[:, :LANES], float(SPARE))
    return jnp.minimum(start, float(SPARE)).astype(i32), cell.astype(i32)


def squeeze(state, bits, axis, roll):
    size = state.shape[axis]
    for bit in range(bits):
        flag = 256 << bit
        ahead = roll(state, size - (1 << bit), axis)
        stay = jnp.where((state & flag) != 0, 0, state)
        state = jnp.where((ahead & flag) != 0, ahead, stay)
    return state


def packing(tally, roll):
    start, cell = land_counts(jnp.where(tally > 0, 0.0, 1.0))
    lane = lax.broadcasted_iota(i32, (ROWS, LANES), 1)
    row = lax.broadcasted_iota(i32, (ROWS, LANES), 0)
    state = jnp.where(tally > 0, ((cell - start) << 8) | 128 | lane, 0)
    state = squeeze(state, 7, 1, roll) & 255
    state = jnp.take_along_axis(state, (lane + start) & 127, axis=1)
    back = (start + lane) >> 7
    rows = jnp.where(state >= 128, (back << 8) | row, 0)
    rows = squeeze(rows, 4, 0, roll) & 31
    return state & 127, rows[:KEPT]


def unpacking(tally):
    start, cell = land_counts(jnp.where(tally > 0, 0.0, 1.0))
    lane = lax.broadcasted_iota(i32, (ROWS, LANES), 1)
    row = lax.broadcasted_iota(i32, (ROWS, LANES), 0)
    return row - ((start + lane) >> 7), (lane - cell) & 127


def pack(rows, lane_from, row_from):
    moved = jnp.take_along_axis(rows, lane_from, axis=1)
    parts = []
    for w in range(KEPT // BAND):
        at = row_from[BAND * w : BAND * w + BAND]
        low = jnp.take_along_axis(moved[BAND * w : BAND * w + BAND], at & 7, axis=0)
        high = jnp.take_along_axis(moved[BAND * w + BAND : BAND * w + 2 * BAND], at & 7, axis=0)
        parts.append(jnp.where(at >= BAND * (w + 1), high, low))
    return jnp.concatenate(parts, axis=0)


def unpack(kept, row_from, lane_from):
    parts = []
    for v in range(ROWS // BAND):
        at = row_from[BAND * v : BAND * v + BAND]
        low = None if v == 0 else jnp.take_along_axis(kept[BAND * v - BAND : BAND * v], at & 7, axis=0)
        high = None if v == KEPT // BAND else jnp.take_along_axis(kept[BAND * v : BAND * v + BAND], at & 7, axis=0)
        if low is None or high is None:
            parts.append(high if low is None else low)
        else:
            parts.append(jnp.where(at >= BAND * v, high, low))
    return jnp.take_along_axis(jnp.concatenate(parts, axis=0), lane_from, axis=1)


def around(ref, band, tier, rims, above=None, below=None):
    lanes = lax.broadcasted_iota(i32, (BAND, LANES), 1)
    row = lax.broadcasted_iota(i32, (BAND, CI), 0)
    here = ref[BAND * band : BAND * band + BAND]
    if above is None:
        above = pltpu.roll(ref[BAND * band + BAND : BAND * band + 2 * BAND], BAND - 1, 0)
    if below is None:
        below = pltpu.roll(ref[BAND * band - BAND : BAND * band], 1, 0)
    north = jnp.where(row == BAND - 1, above, pltpu.roll(here, BAND - 1, 0))
    south = jnp.where(row == 0, below, pltpu.roll(here, 1, 0))
    rim = rims[band]
    east = pltpu.roll(here, CI - 1, 1)
    east_rim = pltpu.roll(rim, 127 - 32 - tier, 1)
    east = jnp.concatenate([east[:, : CI - LANES], jnp.where(lanes == 127, east_rim, east[:, CI - LANES :])], 1)
    west = pltpu.roll(here, 1, 1)
    west_rim = pltpu.roll(rim, LANES - tier, 1)
    west = jnp.concatenate([jnp.where(lanes == 0, west_rim, west[:, :LANES]), west[:, LANES:]], 1)
    return here, north, south, east, west


def divergence(cells, bounds, level):
    here, *others = cells
    total = None
    for bound, other in zip(bounds, others):
        term = jnp.where(bound > level, other - here, 0.0)
        total = term if total is None else total + term
    return total


def exchange(
    warmth, salt, tally, out, lap, depth, least, rims, edges,
    heat, brine, bottom, boxes, pack_lane, pack_row, lane_back, row_back, rim_low, rim_high, brink_out, brink_in, rows_out, rows_in,
    in_sem, send_sem, recv_sem, rim_ssem, rim_rsem, brink_ssem, brink_rsem, row_ssem, row_rsem,
):
    ty = lax.axis_index("ty")
    tx = lax.axis_index("tx")
    outer = jnp.logical_or(tx == 0, tx == LAST)
    barrier = pltpu.get_barrier_semaphore()
    loads = [pltpu.make_async_copy(tally, bottom, in_sem.at[2 * CHUNKS])]
    for chunk in range(CHUNKS):
        part = pl.ds(CUTS[chunk], CUTS[chunk + 1] - CUTS[chunk])
        loads.append(pltpu.make_async_copy(warmth.at[part], heat.at[part], in_sem.at[2 * chunk]))
        loads.append(pltpu.make_async_copy(salt.at[part], brine.at[part], in_sem.at[2 * chunk + 1]))
    loads[0].start()
    for step in range(1, NX):
        pl.semaphore_signal(barrier, inc=1, device_id={"tx": (tx + step) & LAST}, device_id_type=MESH)

    @pl.when(ty > 0)
    def _():
        pl.semaphore_signal(barrier, inc=1, device_id={"ty": ty - 1}, device_id_type=MESH)

    @pl.when(ty < NY - 1)
    def _():
        pl.semaphore_signal(barrier, inc=1, device_id={"ty": ty + 1}, device_id_type=MESH)

    for load in loads[1:]:
        load.start()
    lanes = lax.broadcasted_iota(i32, (BAND, LANES), 1)
    partners = [((tx // 4 + dy) & 3) * 4 + ((tx + dz) & 3) for dy, dz in FAR[:-1]]

    def box_copy(chunk, to, source):
        part = pl.ds(0, ROWS)
        if chunk < CHUNKS:
            part = pl.ds(ROWS + KEPT * CUTS[chunk], KEPT * (CUTS[chunk + 1] - CUTS[chunk]))
        return pltpu.make_async_remote_copy(
            src_ref=boxes.at[to, part], dst_ref=boxes.at[NX + source, part],
            send_sem=send_sem.at[chunk, to], recv_sem=recv_sem.at[chunk, source],
            device_id={"tx": to}, device_id_type=MESH,
        )

    def rim_copy(to, source):
        return pltpu.make_async_remote_copy(
            src_ref=rim_low.at[to], dst_ref=rims.at[source],
            send_sem=rim_ssem.at[to], recv_sem=rim_rsem.at[source],
            device_id={"tx": to}, device_id_type=MESH,
        )

    def brink_copy(to, source):
        side = jnp.where(source == 0, 0, 1)
        return pltpu.make_async_remote_copy(
            src_ref=brink_out.at[to], dst_ref=brink_in.at[side],
            send_sem=brink_ssem.at[to], recv_sem=brink_rsem.at[side],
            device_id={"tx": to}, device_id_type=MESH,
        )

    def find(to):
        at = pl.ds(pl.multiple_of(to * CI, CI), CI)
        deep = bottom[:, at]
        lane_from, row_from = packing(as_rows(deep), pltpu.roll)
        pack_lane[to] = lane_from
        pack_row[to] = row_from
        deep = deep.astype(f32)
        low = pltpu.roll(deep[:, CI - LANES :], TIERS + 1, 1)
        high = pltpu.roll(deep[:, :LANES], 32 + TIERS, 1)
        rim_low[(to + 1) & LAST] = jnp.where(lanes == TIERS, low, 0.0)
        rim_high[(to + LAST) & LAST] = jnp.where(lanes == 32 + TIERS, high, 0.0)

    def make(first, last, step):
        to = partner_of(tx, step)
        slot = jnp.where(step == LAST, NX + to, to)
        east = (to + 1) & LAST
        west = (to + LAST) & LAST
        at = pl.ds(pl.multiple_of(to * CI, CI), CI)
        low = jnp.zeros((BAND, LANES), f32)
        high = jnp.zeros((BAND, LANES), f32)
        lane_from = pack_lane[to]
        row_from = pack_row[to]
        for tier in range(first, last):
            value = density(heat[tier, :, at], brine[tier, :, at], tier)
            boxes[slot, ROWS + KEPT * tier : ROWS + KEPT * tier + KEPT] = pack(as_rows(value), lane_from, row_from)
            low = jnp.where(lanes == tier, pltpu.roll(value[:, CI - LANES :], tier + 1, 1), low)
            high = jnp.where(lanes == 32 + tier, pltpu.roll(value[:, :LANES], 32 + tier, 1), high)
            if tier >= EARLY:
                brink = jnp.where(tx == 0, value[:1], value[BAND - 1 :])
                for v in range(CI // LANES):
                    place = (tier - EARLY) * (CI // LANES) + v
                    brink_out[to, place : place + 1] = brink[:, LANES * v : LANES * v + LANES]
        return east, low, west, high

    def make_two(first, last, pair):
        rims_of = [make(first, last, 2 * pair + n) for n in (0, 1)]
        for east, low, west, high in rims_of:
            rim_low[east] = rim_low[east] + low
            rim_high[west] = rim_high[west] + high

    def wait_loads(chunk):
        loads[1 + 2 * chunk].wait()
        loads[2 + 2 * chunk].wait()

    def make_and_send(first, last, sends, before):
        def one(pair, carry):
            make_two(first, last, pair)

            @pl.when(pair > 0)
            def _():
                if sends is not None:
                    box_copy(sends, partner_of(tx, 2 * pair - 2), tx).start()
                    box_copy(sends, partner_of(tx, 2 * pair - 1), tx).start()

            @pl.when(pair == 0)
            def _():
                if before is not None:
                    box_copy(before, partners[LAST - 1], tx).start()

            return carry

        lax.fori_loop(0, NX // 2, one, 0)

    def find_four(four, carry):
        for n in range(4):
            find(4 * four + n)
        return carry

    def take_tally(to, carry):
        at = pl.ds(pl.multiple_of(to * CI, CI), CI)
        boxes[jnp.where(to == tx, NX + to, to), :ROWS] = as_rows(bottom[:, at]).astype(f32)
        return carry

    loads[0].wait()
    lax.fori_loop(0, NX, take_tally, 0, unroll=4)
    neighbours = jnp.where(ty > 0, 1, 0) + jnp.where(ty < NY - 1, 1, 0)
    pl.semaphore_wait(barrier, NX - 1 + neighbours)
    for to in partners:
        box_copy(CHUNKS, to, tx).start()
    lax.fori_loop(0, NX // 4, find_four, 0)
    wait_loads(0)
    make_and_send(CUTS[0], CUTS[1], 0, None)
    wait_loads(1)
    make_and_send(CUTS[1], CUTS[2], 1, 0)
    wait_loads(2)
    wait_loads(3)
    make_and_send(CUTS[2], CUTS[4], None, 1)

    def join(to, carry):
        rim_low[to] = rim_low[to] + rim_high[to]
        return carry

    lax.fori_loop(0, NX, join, 0)
    rims[tx] = rim_low[tx]

    @pl.when(outer)
    def _():
        brink_in[jnp.where(tx == 0, 0, 1)] = brink_out[tx]
        for to in partners:
            brink_copy(to, tx).start()

    for to in partners:
        rim_copy(to, tx).start()
    for chunk in (2, 3):
        for to in partners:
            box_copy(chunk, to, tx).start()

    def arrive(chunk, source):
        @pl.when(source != tx)
        def _():
            if chunk == 0:
                box_copy(CHUNKS, source, source).wait_recv()
            box_copy(chunk, source, source).wait_recv()

        rows = pl.ds(pl.multiple_of(source * BAND, BAND), BAND)
        deep = boxes[NX + source, :ROWS]
        if chunk == 0:
            row_from, lane_from = unpacking(deep)
            row_back[source] = row_from
            lane_back[source] = lane_from
            deep = as_block(deep)
            depth[rows] = deep
        else:
            row_from = row_back[source]
            lane_from = lane_back[source]
            deep = as_block(deep)
        for tier in range(CUTS[chunk], CUTS[chunk + 1]):
            kept = boxes[NX + source, ROWS + KEPT * tier : ROWS + KEPT * tier + KEPT]
            out[tier, rows] = jnp.where(deep > tier, as_block(unpack(kept, row_from, lane_from)), 0.0)

    def arrive_all(chunk, first=0, last=NX):
        def one(source, carry):
            arrive(chunk, source)
            return carry

        lax.fori_loop(first, last, one, 0)

    def laplace(chunk):
        def one(tier, carry):
            for band in INNER:
                rows = slice(BAND * band, BAND * band + BAND)
                bounds = [least[side, rows] for side in range(4)]
                lap[tier, rows] = divergence(around(out.at[tier], band, tier, rims), bounds, tier.astype(f32))
            return carry

        lax.fori_loop(CUTS[chunk], CUTS[chunk + 1], one, 0)

    arrive_all(0)
    arrive_all(1)

    def rim_in(source, carry):
        @pl.when(source != tx)
        def _():
            rim_copy(source, source).wait_recv()

        return carry

    lax.fori_loop(0, NX, rim_in, 0)
    for band in INNER:
        here, *others = around(depth, band, TIERS, rims)
        for side, other in enumerate(others):
            least[side, BAND * band : BAND * band + BAND] = jnp.minimum(here, other)
    laplace(0)
    laplace(1)

    arrive(2, 0)
    arrive(2, LAST)
    for side, at in ((0, 0), (1, CJ - 1)):
        @pl.when(tx != (LAST if side else 0))
        def _():
            brink_copy(LAST if side else 0, LAST if side else 0).wait_recv()

        for tier in range(EARLY):
            rows_out[side, tier : tier + 1] = out[tier, at : at + 1]
        rows_out[side, TIERS : TIERS + 1] = depth[at : at + 1]
        for place in range((TIERS - EARLY) * CI // LANES):
            tier, v = EARLY + place // (CI // LANES), place % (CI // LANES)
            rows_out[side, tier : tier + 1, LANES * v : LANES * v + LANES] = brink_in[side, place : place + 1]

    arrive(2, 1)

    def row_copy(side, along):
        place = 1 - side if along == "ty" else 1
        if along == "ty":
            device = {"ty": jnp.minimum(ty + 1, NY - 1) if side else jnp.maximum(ty - 1, 0)}
        else:
            device = {"tx": LAST - tx}
        return pltpu.make_async_remote_copy(
            src_ref=rows_out.at[side], dst_ref=rows_in.at[place], send_sem=row_ssem.at[side], recv_sem=row_rsem.at[place],
            device_id=device, device_id_type=MESH,
        )

    @pl.when(ty > 0)
    def _():
        row_copy(0, "ty").start()

    @pl.when(ty < NY - 1)
    def _():
        row_copy(1, "ty").start()

    @pl.when(ty == NY - 1)
    def _():
        row_copy(1, "tx").start()

    arrive_all(2, 2, LAST)
    laplace(2)

    @pl.when(outer)
    def _():
        for to in partners:
            brink_copy(to, tx).wait_send()

    for to in partners:
        rim_copy(to, tx).wait_send()
        for chunk in (CHUNKS, 0, 1, 2):
            box_copy(chunk, to, tx).wait_send()
    arrive_all(3)

    @pl.when(ty > 0)
    def _():
        row_copy(0, "ty").wait_send()
        row_copy(1, "ty").wait_recv()

    @pl.when(ty < NY - 1)
    def _():
        row_copy(1, "ty").wait_send()
        row_copy(0, "ty").wait_recv()

    @pl.when(ty == NY - 1)
    def _():
        row_copy(1, "tx").wait()

    edges[0] = rows_in[0]
    edges[0, TIERS : TIERS + 1] = jnp.where(ty > 0, rows_in[0, TIERS : TIERS + 1], 0.0)
    turn = 127 - lax.broadcasted_iota(i32, (24, LANES), 1)
    upper = rows_in[1]
    flipped = [jnp.take_along_axis(upper[:, LANES * v : LANES * v + LANES], turn, axis=1) for v in (3, 2, 1, 0)]
    edges[1] = jnp.where(ty == NY - 1, jnp.concatenate(flipped, axis=1), upper)

    for to in partners:
        box_copy(3, to, tx).wait_send()


def finish(field, lap, depth, least, rims, edges, field_out, lap_out, ends, late, sem):
    middle = pl.ds(BAND, CJ - 2 * BAND)
    half = TIERS // 2
    copies = [pltpu.make_async_copy(field.at[pl.ds(half * n, half)], field_out.at[pl.ds(half * n, half)], sem.at[n]) for n in (0, 1)]
    copies.append(pltpu.make_async_copy(lap.at[pl.ds(0, EARLY), middle], lap_out.at[pl.ds(0, EARLY), middle], sem.at[2]))
    for copy in copies:
        copy.start()

    def outer(ref, tier, band):
        row = edges[1 if band else 0, tier : tier + 1]
        return around(ref, band, tier, rims, **{"above" if band else "below": row})

    for place, band in enumerate((0, LAST)):
        here, *others = outer(depth, TIERS, band)
        bounds = [jnp.minimum(here, other) for other in others]
        for tier in range(TIERS):
            ends[place, tier] = divergence(outer(field.at[tier], tier, band), bounds, tier)
        copies.append(pltpu.make_async_copy(ends.at[place], lap_out.at[:, pl.ds(BAND * band, BAND)], sem.at[3 + place]))
        copies[-1].start()
    for tier in range(EARLY, TIERS):
        for band in INNER:
            bounds = [least[side, BAND * band : BAND * band + BAND] for side in range(4)]
            late[tier - EARLY, BAND * (band - 1) : BAND * band] = divergence(around(field.at[tier], band, tier, rims), bounds, tier)
    copies.append(pltpu.make_async_copy(late, lap_out.at[pl.ds(EARLY, TIERS - EARLY), middle], sem.at[5]))
    copies[-1].start()
    for copy in copies:
        copy.wait()


def on_device(warmth, salt, tally):
    hbm = pl.BlockSpec(memory_space=pltpu.HBM)
    vmem = pl.BlockSpec(memory_space=pltpu.VMEM)
    held = pl.pallas_call(
        exchange,
        out_shape=(
            pltpu.VMEM((TIERS, CJ, CI), f32),
            pltpu.VMEM((TIERS, CJ, CI), f32),
            pltpu.VMEM((CJ, CI), f32),
            pltpu.VMEM((4, CJ, CI), f32),
            pltpu.VMEM((NX, BAND, LANES), f32),
            pltpu.VMEM((2, 24, CI), f32),
        ),
        in_specs=[hbm] * 3,
        out_specs=(vmem,) * 6,
        scratch_shapes=[
            pltpu.VMEM((TIERS, BAND, COLS), f32),
            pltpu.VMEM((TIERS, BAND, COLS), f32),
            pltpu.VMEM((BAND, COLS), i32),
            pltpu.VMEM((2 * NX, BOX, LANES), f32),
            pltpu.VMEM((NX, ROWS, LANES), i32),
            pltpu.VMEM((NX, KEPT, LANES), i32),
            pltpu.VMEM((NX, ROWS, LANES), i32),
            pltpu.VMEM((NX, ROWS, LANES), i32),
            pltpu.VMEM((NX, BAND, LANES), f32),
            pltpu.VMEM((NX, BAND, LANES), f32),
            pltpu.VMEM((NX, BAND, LANES), f32),
            pltpu.VMEM((2, BAND, LANES), f32),
            pltpu.VMEM((2, 24, CI), f32),
            pltpu.VMEM((2, 24, CI), f32),
            pltpu.SemaphoreType.DMA((2 * CHUNKS + 1,)),
            pltpu.SemaphoreType.DMA((CHUNKS + 1, NX)),
            pltpu.SemaphoreType.DMA((CHUNKS + 1, NX)),
            pltpu.SemaphoreType.DMA((NX,)),
            pltpu.SemaphoreType.DMA((NX,)),
            pltpu.SemaphoreType.DMA((NX,)),
            pltpu.SemaphoreType.DMA((2,)),
            pltpu.SemaphoreType.DMA((2,)),
            pltpu.SemaphoreType.DMA((2,)),
        ],
        compiler_params=pltpu.CompilerParams(collective_id=0, has_side_effects=True, vmem_limit_bytes=48 * 2**20),
        name="exchange",
    )(warmth, salt, tally)
    return pl.pallas_call(
        finish,
        out_shape=(jax.ShapeDtypeStruct((TIERS, CJ, CI), f32),) * 2,
        in_specs=[vmem] * 6,
        out_specs=(hbm,) * 2,
        scratch_shapes=[
            pltpu.VMEM((2, TIERS, BAND, CI), f32),
            pltpu.VMEM((TIERS - EARLY, CJ - 2 * BAND, CI), f32),
            pltpu.SemaphoreType.DMA((6,)),
        ],
        compiler_params=pltpu.CompilerParams(vmem_limit_bytes=16 * 2**20),
        name="finish",
    )(*held)


def solution(mesh):
    placed = (P(None, ("ty", "tx"), None), P(None, ("ty", "tx"), None), P(("ty", "tx"), None))
    return jax.shard_map(
        on_device,
        mesh=mesh,
        in_specs=placed,
        out_specs=(P(None, "ty", "tx"), P(None, "ty", "tx")),
        check_vma=False,
    )
```

```python
import jax
import jax.numpy as jnp
from jax import lax
from jax.experimental import pallas as pl
from jax.experimental.pallas import tpu as pltpu
from jax.sharding import PartitionSpec as P

therm_coef = 0.1655
haline_coef = 0.76554
cabbel_coef = 0.05952
haline_second = 0.00054914
thermo_press = 0.0001497
haline_press = 1.109e-05
cross_coef = 0.0024341

MESH = pl.DeviceIdType.MESH
TIERS = 16
BAND = 8
CJ = 128
CI = 512
NX = 16
NY = 8
COLS = NX * CI
LANES = 128
ROWS = BAND * CI // LANES
KEPT = 24
SPARE = (ROWS - KEPT) * LANES
CUTS = (0, 5, 10, 14, 16)
CHUNKS = len(CUTS) - 1
EARLY = CUTS[-2]
DONE = CUTS[-3]
RIM = ROWS + CUTS[1] * KEPT
BOX = ROWS + TIERS * KEPT + BAND
INNER = range(1, NX - 1)
LAST = NX - 1
FAR = ((0, 2), (2, 2), (0, 1), (1, 1), (3, 3), (0, 3), (2, 1), (2, 3), (1, 2), (3, 2), (1, 3), (3, 1), (2, 0), (1, 0), (3, 0), (0, 0))
f32 = jnp.float32
i32 = jnp.int32


def density(warmth, salt, tier):
    depth = 5.0 + 10.0 * tier
    a = warmth - 10.0
    b = salt - 35.0
    heat = (-therm_coef * (1.0 + thermo_press * depth)) - (0.5 * therm_coef * cabbel_coef) * a - cross_coef * b
    salty = (haline_coef * (1.0 - haline_press * depth)) - (0.5 * haline_coef * haline_second) * b
    return heat * a + salty * b


def partner_of(tx, step, way=1):
    dy = jnp.int32(0)
    dz = jnp.int32(0)
    for number, (far_y, far_z) in enumerate(FAR):
        dy = jnp.where(step == number, far_y, dy)
        dz = jnp.where(step == number, far_z, dz)
    return ((tx // 4 + way * dy) & 3) * 4 + ((tx + way * dz) & 3)


def row_of(tier):
    return ROWS + KEPT * tier + (BAND if tier >= CUTS[1] else 0)


def as_rows(block):
    return jnp.concatenate([block[:, LANES * v : LANES * v + LANES] for v in range(CI // LANES)], axis=0)


def as_block(rows):
    return jnp.concatenate([rows[BAND * v : BAND * v + BAND] for v in range(CI // LANES)], axis=1)


def land_counts(land):
    one = lax.broadcasted_iota(i32, (LANES, 2 * LANES), 0)
    two = lax.broadcasted_iota(i32, (LANES, 2 * LANES), 1)
    ahead = jnp.where(jnp.logical_or(two >= LANES, one < two), 1.0, 0.0).astype(jnp.bfloat16)
    both = jnp.dot(land.astype(jnp.bfloat16), ahead, preferred_element_type=f32)
    one = lax.broadcasted_iota(i32, (ROWS, ROWS), 0)
    two = lax.broadcasted_iota(i32, (ROWS, ROWS), 1)
    above = jnp.where(two < one, 1.0, 0.0).astype(jnp.bfloat16)
    start = jnp.dot(above, both[:, LANES:].astype(jnp.bfloat16), preferred_element_type=f32)
    cell = jnp.minimum(start + both[:, :LANES], float(SPARE))
    return jnp.minimum(start, float(SPARE)).astype(i32), cell.astype(i32)


def squeeze(state, bits, axis, roll):
    size = state.shape[axis]
    for bit in range(bits):
        flag = 256 << bit
        ahead = roll(state, size - (1 << bit), axis)
        stay = jnp.where((state & flag) != 0, 0, state)
        state = jnp.where((ahead & flag) != 0, ahead, stay)
    return state


def packing(tally, roll):
    start, cell = land_counts(jnp.where(tally > 0, 0.0, 1.0))
    lane = lax.broadcasted_iota(i32, (ROWS, LANES), 1)
    row = lax.broadcasted_iota(i32, (ROWS, LANES), 0)
    state = jnp.where(tally > 0, ((cell - start) << 8) | 128 | lane, 0)
    state = squeeze(state, 7, 1, roll) & 255
    state = jnp.take_along_axis(state, (lane + start) & 127, axis=1)
    back = (start + lane) >> 7
    rows = jnp.where(state >= 128, (back << 8) | row, 0)
    rows = squeeze(rows, 4, 0, roll) & 31
    return state & 127, rows[:KEPT]


def unpacking(tally):
    start, cell = land_counts(jnp.where(tally > 0, 0.0, 1.0))
    lane = lax.broadcasted_iota(i32, (ROWS, LANES), 1)
    row = lax.broadcasted_iota(i32, (ROWS, LANES), 0)
    return row - ((start + lane) >> 7), (lane - cell) & 127


def pack(rows, lane_from, row_from):
    moved = jnp.take_along_axis(rows, lane_from, axis=1)
    parts = []
    for w in range(KEPT // BAND):
        at = row_from[BAND * w : BAND * w + BAND]
        low = jnp.take_along_axis(moved[BAND * w : BAND * w + BAND], at & 7, axis=0)
        high = jnp.take_along_axis(moved[BAND * w + BAND : BAND * w + 2 * BAND], at & 7, axis=0)
        parts.append(jnp.where(at >= BAND * (w + 1), high, low))
    return jnp.concatenate(parts, axis=0)


def unpack(kept, row_from, lane_from):
    parts = []
    for v in range(ROWS // BAND):
        at = row_from[BAND * v : BAND * v + BAND]
        low = None if v == 0 else jnp.take_along_axis(kept[BAND * v - BAND : BAND * v], at & 7, axis=0)
        high = None if v == KEPT // BAND else jnp.take_along_axis(kept[BAND * v : BAND * v + BAND], at & 7, axis=0)
        if low is None or high is None:
            parts.append(high if low is None else low)
        else:
            parts.append(jnp.where(at >= BAND * v, high, low))
    return jnp.take_along_axis(jnp.concatenate(parts, axis=0), lane_from, axis=1)


def around(ref, band, tier, rims, above=None, below=None):
    lanes = lax.broadcasted_iota(i32, (BAND, LANES), 1)
    row = lax.broadcasted_iota(i32, (BAND, CI), 0)
    here = ref[BAND * band : BAND * band + BAND]
    if above is None:
        above = pltpu.roll(ref[BAND * band + BAND : BAND * band + 2 * BAND], BAND - 1, 0)
    if below is None:
        below = pltpu.roll(ref[BAND * band - BAND : BAND * band], 1, 0)
    north = jnp.where(row == BAND - 1, above, pltpu.roll(here, BAND - 1, 0))
    south = jnp.where(row == 0, below, pltpu.roll(here, 1, 0))
    rim = rims[band]
    east = pltpu.roll(here, CI - 1, 1)
    east_rim = pltpu.roll(rim, 127 - 32 - tier, 1)
    east = jnp.concatenate([east[:, : CI - LANES], jnp.where(lanes == 127, east_rim, east[:, CI - LANES :])], 1)
    west = pltpu.roll(here, 1, 1)
    west_rim = pltpu.roll(rim, LANES - tier, 1)
    west = jnp.concatenate([jnp.where(lanes == 0, west_rim, west[:, :LANES]), west[:, LANES:]], 1)
    return here, north, south, east, west


def divergence(cells, bounds, level):
    here, *others = cells
    total = None
    for bound, other in zip(bounds, others):
        term = jnp.where(bound > level, other - here, 0.0)
        total = term if total is None else total + term
    return total


def exchange(
    warmth, salt, tally, out, lap, depth, least, rims, edges,
    heat, brine, bottom, boxes, pack_lane, pack_row, lane_back, row_back, brink_out, brink_in, rows_out, rows_in,
    in_sem, send_sem, recv_sem, brink_ssem, brink_rsem, row_ssem, row_rsem,
):
    ty = lax.axis_index("ty")
    tx = lax.axis_index("tx")
    outer = jnp.logical_or(tx == 0, tx == LAST)
    barrier = pltpu.get_barrier_semaphore()
    loads = [pltpu.make_async_copy(tally, bottom, in_sem.at[2 * CHUNKS])]
    for chunk in range(CHUNKS):
        part = pl.ds(CUTS[chunk], CUTS[chunk + 1] - CUTS[chunk])
        loads.append(pltpu.make_async_copy(warmth.at[part], heat.at[part], in_sem.at[2 * chunk]))
        loads.append(pltpu.make_async_copy(salt.at[part], brine.at[part], in_sem.at[2 * chunk + 1]))
    loads[0].start()
    for step in range(1, NX):
        pl.semaphore_signal(barrier, inc=1, device_id={"tx": (tx + step) & LAST}, device_id_type=MESH)

    @pl.when(ty > 0)
    def _():
        pl.semaphore_signal(barrier, inc=1, device_id={"ty": ty - 1}, device_id_type=MESH)

    @pl.when(ty < NY - 1)
    def _():
        pl.semaphore_signal(barrier, inc=1, device_id={"ty": ty + 1}, device_id_type=MESH)

    for load in loads[1:]:
        load.start()
    lanes = lax.broadcasted_iota(i32, (BAND, LANES), 1)
    partners = [((tx // 4 + dy) & 3) * 4 + ((tx + dz) & 3) for dy, dz in FAR[:-1]]

    def box_copy(chunk, to, source):
        part = pl.ds(0, ROWS)
        if chunk < CHUNKS:
            first = RIM if chunk == 1 else row_of(CUTS[chunk])
            part = pl.ds(first, row_of(CUTS[chunk + 1] - 1) + KEPT - first)
        return pltpu.make_async_remote_copy(
            src_ref=boxes.at[to, part], dst_ref=boxes.at[NX + source, part],
            send_sem=send_sem.at[chunk, to], recv_sem=recv_sem.at[chunk, source],
            device_id={"tx": to}, device_id_type=MESH,
        )

    def brink_copy(to, source):
        side = jnp.where(source == 0, 0, 1)
        return pltpu.make_async_remote_copy(
            src_ref=brink_out.at[to], dst_ref=brink_in.at[side],
            send_sem=brink_ssem.at[to], recv_sem=brink_rsem.at[side],
            device_id={"tx": to}, device_id_type=MESH,
        )

    def find(to):
        at = pl.ds(pl.multiple_of(to * CI, CI), CI)
        lane_from, row_from = packing(as_rows(bottom[:, at]), pltpu.roll)
        pack_lane[to] = lane_from
        pack_row[to] = row_from
        return lane_from, row_from

    def make_rim(to):
        west = pl.ds(pl.multiple_of(((to * CI) + COLS - LANES) & (COLS - 1), LANES), LANES)
        east = pl.ds(pl.multiple_of(((to * CI) + CI) & (COLS - 1), LANES), LANES)
        rim = pltpu.roll(bottom[:, west].astype(f32), TIERS + 1, 1)
        rim = jnp.where(lanes == 32 + TIERS, pltpu.roll(bottom[:, east].astype(f32), 32 + TIERS, 1), rim)
        for tier in range(TIERS):
            low = density(heat[tier, :, west], brine[tier, :, west], tier)
            high = density(heat[tier, :, east], brine[tier, :, east], tier)
            rim = jnp.where(lanes == tier, pltpu.roll(low, tier + 1, 1), rim)
            rim = jnp.where(lanes == 32 + tier, pltpu.roll(high, 32 + tier, 1), rim)
        boxes[jnp.where(to == tx, NX + to, to), RIM : RIM + BAND] = rim

    def make(first, last, step):
        to = partner_of(tx, step)
        slot = jnp.where(step == LAST, NX + to, to)
        at = pl.ds(pl.multiple_of(to * CI, CI), CI)
        lane_from, row_from = find(to) if first == 0 else (pack_lane[to], pack_row[to])
        for tier in range(first, last):
            value = density(heat[tier, :, at], brine[tier, :, at], tier)
            boxes[slot, row_of(tier) : row_of(tier) + KEPT] = pack(as_rows(value), lane_from, row_from)
            if tier >= EARLY:
                brink = jnp.where(tx == 0, value[:1], value[BAND - 1 :])
                for v in range(CI // LANES):
                    place = (tier - EARLY) * (CI // LANES) + v
                    brink_out[to, place : place + 1] = brink[:, LANES * v : LANES * v + LANES]

    def make_two(first, last, pair):
        for n in (0, 1):
            make(first, last, 2 * pair + n)

    def wait_loads(chunk):
        loads[1 + 2 * chunk].wait()
        loads[2 + 2 * chunk].wait()

    def make_and_send(first, last, sends, before):
        def one(pair, carry):
            make_two(first, last, pair)

            @pl.when(pair > 0)
            def _():
                if sends is not None:
                    box_copy(sends, partner_of(tx, 2 * pair - 2), tx).start()
                    box_copy(sends, partner_of(tx, 2 * pair - 1), tx).start()

            @pl.when(pair == 0)
            def _():
                if before is not None:
                    box_copy(before, partners[LAST - 1], tx).start()

            return carry

        lax.fori_loop(0, NX // 2, one, 0)

    def take_tally(to, carry):
        at = pl.ds(pl.multiple_of(to * CI, CI), CI)
        boxes[jnp.where(to == tx, NX + to, to), :ROWS] = as_rows(bottom[:, at]).astype(f32)
        return carry

    loads[0].wait()
    lax.fori_loop(0, NX, take_tally, 0, unroll=4)
    neighbours = jnp.where(ty > 0, 1, 0) + jnp.where(ty < NY - 1, 1, 0)
    pl.semaphore_wait(barrier, NX - 1 + neighbours)
    for to in partners:
        box_copy(CHUNKS, to, tx).start()
    wait_loads(0)
    make_and_send(CUTS[0], CUTS[1], 0, None)
    for chunk in range(1, CHUNKS):
        wait_loads(chunk)

    def rim_two(pair, carry):
        make_rim(2 * pair)
        make_rim(2 * pair + 1)
        return carry

    lax.fori_loop(0, NX // 2, rim_two, 0)
    box_copy(0, partners[LAST - 1], tx).start()
    make_and_send(CUTS[1], CUTS[2], 1, None)
    make_and_send(CUTS[2], CUTS[4], None, 1)

    @pl.when(outer)
    def _():
        brink_in[jnp.where(tx == 0, 0, 1)] = brink_out[tx]
        for to in partners:
            brink_copy(to, tx).start()

    for chunk in (2, 3):
        for to in partners:
            box_copy(chunk, to, tx).start()

    def arrive(chunk, source):
        @pl.when(source != tx)
        def _():
            if chunk == 0:
                box_copy(CHUNKS, source, source).wait_recv()
            box_copy(chunk, source, source).wait_recv()

        rows = pl.ds(pl.multiple_of(source * BAND, BAND), BAND)
        deep = boxes[NX + source, :ROWS]
        if chunk == 0:
            row_from, lane_from = unpacking(deep)
            row_back[source] = row_from
            lane_back[source] = lane_from
            deep = as_block(deep)
            depth[rows] = deep
        else:
            row_from = row_back[source]
            lane_from = lane_back[source]
            deep = as_block(deep)
        if chunk == 1:
            rims[source] = boxes[NX + source, RIM : RIM + BAND]
        for tier in range(CUTS[chunk], CUTS[chunk + 1]):
            kept = boxes[NX + source, row_of(tier) : row_of(tier) + KEPT]
            out[tier, rows] = jnp.where(deep > tier, as_block(unpack(kept, row_from, lane_from)), 0.0)

    def arrive_all(chunk):
        def one(step, carry):
            arrive(chunk, partner_of(tx, (step + LAST) & LAST, -1))
            return carry

        lax.fori_loop(0, NX, one, 0)

    def laplace(chunk):
        def one(tier, carry):
            for band in INNER:
                rows = slice(BAND * band, BAND * band + BAND)
                bounds = [least[side, rows] for side in range(4)]
                lap[tier, rows] = divergence(around(out.at[tier], band, tier, rims), bounds, tier.astype(f32))
            return carry

        lax.fori_loop(CUTS[chunk], CUTS[chunk + 1], one, 0)

    arrive_all(0)
    arrive_all(1)

    for band in INNER:
        here, *others = around(depth, band, TIERS, rims)
        for side, other in enumerate(others):
            least[side, BAND * band : BAND * band + BAND] = jnp.minimum(here, other)
    laplace(0)
    laplace(1)

    arrive_all(2)
    for side, at in ((0, 0), (1, CJ - 1)):
        @pl.when(tx != (LAST if side else 0))
        def _():
            brink_copy(LAST if side else 0, LAST if side else 0).wait_recv()

        for tier in range(EARLY):
            rows_out[side, tier : tier + 1] = out[tier, at : at + 1]
        rows_out[side, TIERS : TIERS + 1] = depth[at : at + 1]
        for place in range((TIERS - EARLY) * CI // LANES):
            tier, v = EARLY + place // (CI // LANES), place % (CI // LANES)
            rows_out[side, tier : tier + 1, LANES * v : LANES * v + LANES] = brink_in[side, place : place + 1]

    def row_copy(side, along):
        place = 1 - side if along == "ty" else 1
        if along == "ty":
            device = {"ty": jnp.minimum(ty + 1, NY - 1) if side else jnp.maximum(ty - 1, 0)}
        else:
            device = {"tx": LAST - tx}
        return pltpu.make_async_remote_copy(
            src_ref=rows_out.at[side], dst_ref=rows_in.at[place], send_sem=row_ssem.at[side], recv_sem=row_rsem.at[place],
            device_id=device, device_id_type=MESH,
        )

    @pl.when(outer)
    def _():
        for to in partners:
            brink_copy(to, tx).wait_send()

    for to in partners:
        for chunk in (CHUNKS, 0, 1):
            box_copy(chunk, to, tx).wait_send()

    @pl.when(ty > 0)
    def _():
        row_copy(0, "ty").start()

    @pl.when(ty < NY - 1)
    def _():
        row_copy(1, "ty").start()

    @pl.when(ty == NY - 1)
    def _():
        row_copy(1, "tx").start()

    for to in partners:
        box_copy(2, to, tx).wait_send()
    arrive_all(3)

    @pl.when(ty > 0)
    def _():
        row_copy(0, "ty").wait_send()
        row_copy(1, "ty").wait_recv()

    @pl.when(ty < NY - 1)
    def _():
        row_copy(1, "ty").wait_send()
        row_copy(0, "ty").wait_recv()

    @pl.when(ty == NY - 1)
    def _():
        row_copy(1, "tx").wait()

    edges[0] = rows_in[0]
    edges[0, TIERS : TIERS + 1] = jnp.where(ty > 0, rows_in[0, TIERS : TIERS + 1], 0.0)
    turn = 127 - lax.broadcasted_iota(i32, (24, LANES), 1)
    upper = rows_in[1]
    flipped = [jnp.take_along_axis(upper[:, LANES * v : LANES * v + LANES], turn, axis=1) for v in (3, 2, 1, 0)]
    edges[1] = jnp.where(ty == NY - 1, jnp.concatenate(flipped, axis=1), upper)

    for to in partners:
        box_copy(3, to, tx).wait_send()


def finish(field, lap, depth, least, rims, edges, field_out, lap_out, ends, late, sem):
    middle = pl.ds(BAND, CJ - 2 * BAND)
    half = TIERS // 2
    copies = [pltpu.make_async_copy(field.at[pl.ds(half * n, half)], field_out.at[pl.ds(half * n, half)], sem.at[n]) for n in (0, 1)]
    copies.append(pltpu.make_async_copy(lap.at[pl.ds(0, DONE), middle], lap_out.at[pl.ds(0, DONE), middle], sem.at[2]))
    for copy in copies:
        copy.start()

    def outer(ref, tier, band):
        row = edges[1 if band else 0, tier : tier + 1]
        return around(ref, band, tier, rims, **{"above" if band else "below": row})

    for place, band in enumerate((0, LAST)):
        here, *others = outer(depth, TIERS, band)
        bounds = [jnp.minimum(here, other) for other in others]
        for tier in range(TIERS):
            ends[place, tier] = divergence(outer(field.at[tier], tier, band), bounds, tier)
        copies.append(pltpu.make_async_copy(ends.at[place], lap_out.at[:, pl.ds(BAND * band, BAND)], sem.at[3 + place]))
        copies[-1].start()
    for part in range((TIERS - DONE) // 2):
        for tier in (DONE + 2 * part, DONE + 2 * part + 1):
            for band in INNER:
                bounds = [least[side, BAND * band : BAND * band + BAND] for side in range(4)]
                late[tier - DONE, BAND * (band - 1) : BAND * band] = divergence(around(field.at[tier], band, tier, rims), bounds, tier)
        two = pl.ds(DONE + 2 * part, 2)
        copies.append(pltpu.make_async_copy(late.at[pl.ds(2 * part, 2)], lap_out.at[two, middle], sem.at[5 + part]))
        copies[-1].start()
    for copy in copies:
        copy.wait()


def on_device(warmth, salt, tally):
    hbm = pl.BlockSpec(memory_space=pltpu.HBM)
    vmem = pl.BlockSpec(memory_space=pltpu.VMEM)
    held = pl.pallas_call(
        exchange,
        out_shape=(
            pltpu.VMEM((TIERS, CJ, CI), f32),
            pltpu.VMEM((TIERS, CJ, CI), f32),
            pltpu.VMEM((CJ, CI), f32),
            pltpu.VMEM((4, CJ, CI), f32),
            pltpu.VMEM((NX, BAND, LANES), f32),
            pltpu.VMEM((2, 24, CI), f32),
        ),
        in_specs=[hbm] * 3,
        out_specs=(vmem,) * 6,
        scratch_shapes=[
            pltpu.VMEM((TIERS, BAND, COLS), f32),
            pltpu.VMEM((TIERS, BAND, COLS), f32),
            pltpu.VMEM((BAND, COLS), i32),
            pltpu.VMEM((2 * NX, BOX, LANES), f32),
            pltpu.VMEM((NX, ROWS, LANES), i32),
            pltpu.VMEM((NX, KEPT, LANES), i32),
            pltpu.VMEM((NX, ROWS, LANES), i32),
            pltpu.VMEM((NX, ROWS, LANES), i32),
            pltpu.VMEM((NX, BAND, LANES), f32),
            pltpu.VMEM((2, BAND, LANES), f32),
            pltpu.VMEM((2, 24, CI), f32),
            pltpu.VMEM((2, 24, CI), f32),
            pltpu.SemaphoreType.DMA((2 * CHUNKS + 1,)),
            pltpu.SemaphoreType.DMA((CHUNKS + 1, NX)),
            pltpu.SemaphoreType.DMA((CHUNKS + 1, NX)),
            pltpu.SemaphoreType.DMA((NX,)),
            pltpu.SemaphoreType.DMA((2,)),
            pltpu.SemaphoreType.DMA((2,)),
            pltpu.SemaphoreType.DMA((2,)),
        ],
        compiler_params=pltpu.CompilerParams(collective_id=0, has_side_effects=True, vmem_limit_bytes=48 * 2**20),
        name="exchange",
    )(warmth, salt, tally)
    return pl.pallas_call(
        finish,
        out_shape=(jax.ShapeDtypeStruct((TIERS, CJ, CI), f32),) * 2,
        in_specs=[vmem] * 6,
        out_specs=(hbm,) * 2,
        scratch_shapes=[
            pltpu.VMEM((2, TIERS, BAND, CI), f32),
            pltpu.VMEM((TIERS - DONE, CJ - 2 * BAND, CI), f32),
            pltpu.SemaphoreType.DMA((5 + (TIERS - DONE) // 2,)),
        ],
        compiler_params=pltpu.CompilerParams(vmem_limit_bytes=16 * 2**20),
        name="finish",
    )(*held)


def solution(mesh):
    placed = (P(None, ("ty", "tx"), None), P(None, ("ty", "tx"), None), P(("ty", "tx"), None))
    return jax.shard_map(
        on_device,
        mesh=mesh,
        in_specs=placed,
        out_specs=(P(None, "ty", "tx"), P(None, "ty", "tx")),
        check_vma=False,
    )
```

```python
import jax
import jax.numpy as jnp
from jax import lax
from jax.experimental import pallas as pl
from jax.experimental.pallas import tpu as pltpu
from jax.sharding import PartitionSpec as P

therm_coef = 0.1655
haline_coef = 0.76554
cabbel_coef = 0.05952
haline_second = 0.00054914
thermo_press = 0.0001497
haline_press = 1.109e-05
cross_coef = 0.0024341

MESH = pl.DeviceIdType.MESH
TIERS = 16
BAND = 8
CJ = 128
CI = 512
NX = 16
NY = 8
COLS = NX * CI
LANES = 128
ROWS = BAND * CI // LANES
KEPT = 24
SPARE = (ROWS - KEPT) * LANES
CUTS = (0, 6, 10, 14, 16)
CHUNKS = len(CUTS) - 1
EARLY = CUTS[-2]
DONE = CUTS[-3]
RIM = ROWS + CUTS[1] * KEPT
BOX = ROWS + TIERS * KEPT + BAND
INNER = range(1, NX - 1)
LAST = NX - 1
ZFIRST = ((0, 2), (2, 2), (0, 1), (1, 1), (3, 3), (0, 3), (2, 1), (2, 3), (1, 2), (3, 2), (1, 3), (3, 1), (2, 0), (1, 0), (3, 0), (0, 0))
FARFIRST = ((2, 2), (2, 1), (2, 3), (1, 2), (3, 2), (1, 1), (3, 3), (1, 3), (3, 1), (2, 0), (0, 2), (1, 0), (3, 0), (0, 1), (0, 3), (0, 0))
ORDERS = (ZFIRST, FARFIRST, FARFIRST, FARFIRST, ZFIRST)
f32 = jnp.float32
i32 = jnp.int32


def density(warmth, salt, tier):
    depth = 5.0 + 10.0 * tier
    a = warmth - 10.0
    b = salt - 35.0
    heat = (-therm_coef * (1.0 + thermo_press * depth)) - (0.5 * therm_coef * cabbel_coef) * a - cross_coef * b
    salty = (haline_coef * (1.0 - haline_press * depth)) - (0.5 * haline_coef * haline_second) * b
    return heat * a + salty * b


def partner_of(tx, step, chunk, way=1):
    dy = jnp.int32(0)
    dz = jnp.int32(0)
    for number, (far_y, far_z) in enumerate(ORDERS[chunk]):
        dy = jnp.where(step == number, far_y, dy)
        dz = jnp.where(step == number, far_z, dz)
    return ((tx // 4 + way * dy) & 3) * 4 + ((tx + way * dz) & 3)


def row_of(tier):
    return ROWS + KEPT * tier + (BAND if tier >= CUTS[1] else 0)


def as_rows(block):
    return jnp.concatenate([block[:, LANES * v : LANES * v + LANES] for v in range(CI // LANES)], axis=0)


def as_block(rows):
    return jnp.concatenate([rows[BAND * v : BAND * v + BAND] for v in range(CI // LANES)], axis=1)


def land_counts(land):
    one = lax.broadcasted_iota(i32, (LANES, 2 * LANES), 0)
    two = lax.broadcasted_iota(i32, (LANES, 2 * LANES), 1)
    ahead = jnp.where(jnp.logical_or(two >= LANES, one < two), 1.0, 0.0).astype(jnp.bfloat16)
    both = jnp.dot(land.astype(jnp.bfloat16), ahead, preferred_element_type=f32)
    one = lax.broadcasted_iota(i32, (ROWS, ROWS), 0)
    two = lax.broadcasted_iota(i32, (ROWS, ROWS), 1)
    above = jnp.where(two < one, 1.0, 0.0).astype(jnp.bfloat16)
    start = jnp.dot(above, both[:, LANES:].astype(jnp.bfloat16), preferred_element_type=f32)
    cell = jnp.minimum(start + both[:, :LANES], float(SPARE))
    return jnp.minimum(start, float(SPARE)).astype(i32), cell.astype(i32)


def squeeze(state, bits, axis, roll):
    size = state.shape[axis]
    for bit in range(bits):
        flag = 256 << bit
        ahead = roll(state, size - (1 << bit), axis)
        stay = jnp.where((state & flag) != 0, 0, state)
        state = jnp.where((ahead & flag) != 0, ahead, stay)
    return state


def packing(tally, roll):
    start, cell = land_counts(jnp.where(tally > 0, 0.0, 1.0))
    lane = lax.broadcasted_iota(i32, (ROWS, LANES), 1)
    row = lax.broadcasted_iota(i32, (ROWS, LANES), 0)
    state = jnp.where(tally > 0, ((cell - start) << 8) | 128 | lane, 0)
    state = squeeze(state, 7, 1, roll) & 255
    state = jnp.take_along_axis(state, (lane + start) & 127, axis=1)
    back = (start + lane) >> 7
    rows = jnp.where(state >= 128, (back << 8) | row, 0)
    rows = squeeze(rows, 4, 0, roll) & 31
    return state & 127, rows[:KEPT]


def unpacking(tally):
    start, cell = land_counts(jnp.where(tally > 0, 0.0, 1.0))
    lane = lax.broadcasted_iota(i32, (ROWS, LANES), 1)
    row = lax.broadcasted_iota(i32, (ROWS, LANES), 0)
    return row - ((start + lane) >> 7), (lane - cell) & 127


def pack(rows, lane_from, row_from):
    moved = jnp.take_along_axis(rows, lane_from, axis=1)
    parts = []
    for w in range(KEPT // BAND):
        at = row_from[BAND * w : BAND * w + BAND]
        low = jnp.take_along_axis(moved[BAND * w : BAND * w + BAND], at & 7, axis=0)
        high = jnp.take_along_axis(moved[BAND * w + BAND : BAND * w + 2 * BAND], at & 7, axis=0)
        parts.append(jnp.where(at >= BAND * (w + 1), high, low))
    return jnp.concatenate(parts, axis=0)


def unpack(kept, row_from, lane_from):
    parts = []
    for v in range(ROWS // BAND):
        at = row_from[BAND * v : BAND * v + BAND]
        low = None if v == 0 else jnp.take_along_axis(kept[BAND * v - BAND : BAND * v], at & 7, axis=0)
        high = None if v == KEPT // BAND else jnp.take_along_axis(kept[BAND * v : BAND * v + BAND], at & 7, axis=0)
        if low is None or high is None:
            parts.append(high if low is None else low)
        else:
            parts.append(jnp.where(at >= BAND * v, high, low))
    return jnp.take_along_axis(jnp.concatenate(parts, axis=0), lane_from, axis=1)


def around(ref, band, tier, rims, above=None, below=None):
    lanes = lax.broadcasted_iota(i32, (BAND, LANES), 1)
    row = lax.broadcasted_iota(i32, (BAND, CI), 0)
    here = ref[BAND * band : BAND * band + BAND]
    if above is None:
        above = pltpu.roll(ref[BAND * band + BAND : BAND * band + 2 * BAND], BAND - 1, 0)
    if below is None:
        below = pltpu.roll(ref[BAND * band - BAND : BAND * band], 1, 0)
    north = jnp.where(row == BAND - 1, above, pltpu.roll(here, BAND - 1, 0))
    south = jnp.where(row == 0, below, pltpu.roll(here, 1, 0))
    rim = rims[band]
    east = pltpu.roll(here, CI - 1, 1)
    east_rim = pltpu.roll(rim, 127 - 32 - tier, 1)
    east = jnp.concatenate([east[:, : CI - LANES], jnp.where(lanes == 127, east_rim, east[:, CI - LANES :])], 1)
    west = pltpu.roll(here, 1, 1)
    west_rim = pltpu.roll(rim, LANES - tier, 1)
    west = jnp.concatenate([jnp.where(lanes == 0, west_rim, west[:, :LANES]), west[:, LANES:]], 1)
    return here, north, south, east, west


def divergence(cells, bounds, level):
    here, *others = cells
    total = None
    for bound, other in zip(bounds, others):
        term = jnp.where(bound > level, other - here, 0.0)
        total = term if total is None else total + term
    return total


def exchange(
    warmth, salt, tally, out, lap, depth, least, rims, edges,
    heat, brine, bottom, boxes, pack_lane, pack_row, lane_back, row_back, brink_out, brink_in, rows_out, rows_in,
    in_sem, send_sem, recv_sem, brink_ssem, brink_rsem, row_ssem, row_rsem,
):
    ty = lax.axis_index("ty")
    tx = lax.axis_index("tx")
    outer = jnp.logical_or(tx == 0, tx == LAST)
    barrier = pltpu.get_barrier_semaphore()
    loads = [pltpu.make_async_copy(tally, bottom, in_sem.at[2 * CHUNKS])]
    for chunk in range(CHUNKS):
        part = pl.ds(CUTS[chunk], CUTS[chunk + 1] - CUTS[chunk])
        loads.append(pltpu.make_async_copy(warmth.at[part], heat.at[part], in_sem.at[2 * chunk]))
        loads.append(pltpu.make_async_copy(salt.at[part], brine.at[part], in_sem.at[2 * chunk + 1]))
    loads[0].start()
    for step in range(1, NX):
        pl.semaphore_signal(barrier, inc=1, device_id={"tx": (tx + step) & LAST}, device_id_type=MESH)

    @pl.when(ty > 0)
    def _():
        pl.semaphore_signal(barrier, inc=1, device_id={"ty": ty - 1}, device_id_type=MESH)

    @pl.when(ty < NY - 1)
    def _():
        pl.semaphore_signal(barrier, inc=1, device_id={"ty": ty + 1}, device_id_type=MESH)

    for load in loads[1:]:
        load.start()
    lanes = lax.broadcasted_iota(i32, (BAND, LANES), 1)
    partners = [[((tx // 4 + dy) & 3) * 4 + ((tx + dz) & 3) for dy, dz in order[:-1]] for order in ORDERS]

    def box_copy(chunk, to, source):
        part = pl.ds(0, ROWS)
        if chunk < CHUNKS:
            first = RIM if chunk == 1 else row_of(CUTS[chunk])
            part = pl.ds(first, row_of(CUTS[chunk + 1] - 1) + KEPT - first)
        return pltpu.make_async_remote_copy(
            src_ref=boxes.at[to, part], dst_ref=boxes.at[NX + source, part],
            send_sem=send_sem.at[chunk, to], recv_sem=recv_sem.at[chunk, source],
            device_id={"tx": to}, device_id_type=MESH,
        )

    def brink_copy(to, source):
        side = jnp.where(source == 0, 0, 1)
        return pltpu.make_async_remote_copy(
            src_ref=brink_out.at[to], dst_ref=brink_in.at[side],
            send_sem=brink_ssem.at[to], recv_sem=brink_rsem.at[side],
            device_id={"tx": to}, device_id_type=MESH,
        )

    def find(to):
        at = pl.ds(pl.multiple_of(to * CI, CI), CI)
        lane_from, row_from = packing(as_rows(bottom[:, at]), pltpu.roll)
        pack_lane[to] = lane_from
        pack_row[to] = row_from
        return lane_from, row_from

    def make_rim(to):
        west = pl.ds(pl.multiple_of(((to * CI) + COLS - LANES) & (COLS - 1), LANES), LANES)
        east = pl.ds(pl.multiple_of(((to * CI) + CI) & (COLS - 1), LANES), LANES)
        rim = pltpu.roll(bottom[:, west].astype(f32), TIERS + 1, 1)
        rim = jnp.where(lanes == 32 + TIERS, pltpu.roll(bottom[:, east].astype(f32), 32 + TIERS, 1), rim)
        for tier in range(TIERS):
            low = density(heat[tier, :, west], brine[tier, :, west], tier)
            high = density(heat[tier, :, east], brine[tier, :, east], tier)
            rim = jnp.where(lanes == tier, pltpu.roll(low, tier + 1, 1), rim)
            rim = jnp.where(lanes == 32 + tier, pltpu.roll(high, 32 + tier, 1), rim)
        boxes[jnp.where(to == tx, NX + to, to), RIM : RIM + BAND] = rim

    def make(first, last, step):
        to = partner_of(tx, step, CUTS.index(first))
        slot = jnp.where(step == LAST, NX + to, to)
        at = pl.ds(pl.multiple_of(to * CI, CI), CI)
        lane_from, row_from = find(to) if first == 0 else (pack_lane[to], pack_row[to])
        for tier in range(first, last):
            value = density(heat[tier, :, at], brine[tier, :, at], tier)
            boxes[slot, row_of(tier) : row_of(tier) + KEPT] = pack(as_rows(value), lane_from, row_from)
            if tier >= EARLY:
                brink = jnp.where(tx == 0, value[:1], value[BAND - 1 :])
                for v in range(CI // LANES):
                    place = (tier - EARLY) * (CI // LANES) + v
                    brink_out[to, place : place + 1] = brink[:, LANES * v : LANES * v + LANES]

    def make_two(first, last, pair):
        for n in (0, 1):
            make(first, last, 2 * pair + n)

    def wait_loads(chunk):
        loads[1 + 2 * chunk].wait()
        loads[2 + 2 * chunk].wait()

    def make_and_send(first, last, sends, before):
        def one(pair, carry):
            make_two(first, last, pair)

            @pl.when(pair > 0)
            def _():
                if sends is not None:
                    box_copy(sends, partner_of(tx, 2 * pair - 2, sends), tx).start()
                    box_copy(sends, partner_of(tx, 2 * pair - 1, sends), tx).start()

            @pl.when(pair == 0)
            def _():
                if before is not None:
                    box_copy(before, partners[before][LAST - 1], tx).start()

            return carry

        lax.fori_loop(0, NX // 2, one, 0)

    def take_tally(to, carry):
        at = pl.ds(pl.multiple_of(to * CI, CI), CI)
        boxes[jnp.where(to == tx, NX + to, to), :ROWS] = as_rows(bottom[:, at]).astype(f32)
        return carry

    loads[0].wait()
    lax.fori_loop(0, NX, take_tally, 0, unroll=4)
    neighbours = jnp.where(ty > 0, 1, 0) + jnp.where(ty < NY - 1, 1, 0)
    pl.semaphore_wait(barrier, NX - 1 + neighbours)
    for to in partners[CHUNKS]:
        box_copy(CHUNKS, to, tx).start()
    wait_loads(0)
    make_and_send(CUTS[0], CUTS[1], 0, None)
    for chunk in range(1, CHUNKS):
        wait_loads(chunk)

    def rim_two(pair, carry):
        make_rim(2 * pair)
        make_rim(2 * pair + 1)
        return carry

    lax.fori_loop(0, NX // 2, rim_two, 0)
    box_copy(0, partners[0][LAST - 1], tx).start()
    make_and_send(CUTS[1], CUTS[2], 1, None)
    make_and_send(CUTS[2], CUTS[4], None, 1)

    @pl.when(outer)
    def _():
        brink_in[jnp.where(tx == 0, 0, 1)] = brink_out[tx]
        for to in partners[0]:
            brink_copy(to, tx).start()

    for chunk in (2, 3):
        for to in partners[chunk]:
            box_copy(chunk, to, tx).start()

    def arrive(chunk, source):
        @pl.when(source != tx)
        def _():
            if chunk == 0:
                box_copy(CHUNKS, source, source).wait_recv()
            box_copy(chunk, source, source).wait_recv()

        rows = pl.ds(pl.multiple_of(source * BAND, BAND), BAND)
        deep = boxes[NX + source, :ROWS]
        if chunk == 0:
            row_from, lane_from = unpacking(deep)
            row_back[source] = row_from
            lane_back[source] = lane_from
            deep = as_block(deep)
            depth[rows] = deep
        else:
            row_from = row_back[source]
            lane_from = lane_back[source]
            deep = as_block(deep)
        if chunk == 1:
            rims[source] = boxes[NX + source, RIM : RIM + BAND]
        for tier in range(CUTS[chunk], CUTS[chunk + 1]):
            kept = boxes[NX + source, row_of(tier) : row_of(tier) + KEPT]
            out[tier, rows] = jnp.where(deep > tier, as_block(unpack(kept, row_from, lane_from)), 0.0)

    def arrive_all(chunk):
        def one(step, carry):
            arrive(chunk, partner_of(tx, (step + LAST) & LAST, chunk, -1))
            return carry

        lax.fori_loop(0, NX, one, 0)

    def laplace(chunk):
        def one(tier, carry):
            for band in INNER:
                rows = slice(BAND * band, BAND * band + BAND)
                bounds = [least[side, rows] for side in range(4)]
                lap[tier, rows] = divergence(around(out.at[tier], band, tier, rims), bounds, tier.astype(f32))
            return carry

        lax.fori_loop(CUTS[chunk], CUTS[chunk + 1], one, 0)

    arrive_all(0)
    arrive_all(1)

    for band in INNER:
        here, *others = around(depth, band, TIERS, rims)
        for side, other in enumerate(others):
            least[side, BAND * band : BAND * band + BAND] = jnp.minimum(here, other)
    laplace(0)
    laplace(1)

    arrive_all(2)
    for side, at in ((0, 0), (1, CJ - 1)):
        @pl.when(tx != (LAST if side else 0))
        def _():
            brink_copy(LAST if side else 0, LAST if side else 0).wait_recv()

        for tier in range(EARLY):
            rows_out[side, tier : tier + 1] = out[tier, at : at + 1]
        rows_out[side, TIERS : TIERS + 1] = depth[at : at + 1]
        for place in range((TIERS - EARLY) * CI // LANES):
            tier, v = EARLY + place // (CI // LANES), place % (CI // LANES)
            rows_out[side, tier : tier + 1, LANES * v : LANES * v + LANES] = brink_in[side, place : place + 1]

    def row_copy(side, along):
        place = 1 - side if along == "ty" else 1
        if along == "ty":
            device = {"ty": jnp.minimum(ty + 1, NY - 1) if side else jnp.maximum(ty - 1, 0)}
        else:
            device = {"tx": LAST - tx}
        return pltpu.make_async_remote_copy(
            src_ref=rows_out.at[side], dst_ref=rows_in.at[place], send_sem=row_ssem.at[side], recv_sem=row_rsem.at[place],
            device_id=device, device_id_type=MESH,
        )

    @pl.when(outer)
    def _():
        for to in partners[0]:
            brink_copy(to, tx).wait_send()

    for to in partners[0]:
        for chunk in (CHUNKS, 0, 1):
            box_copy(chunk, to, tx).wait_send()

    @pl.when(ty > 0)
    def _():
        row_copy(0, "ty").start()

    @pl.when(ty < NY - 1)
    def _():
        row_copy(1, "ty").start()

    @pl.when(ty == NY - 1)
    def _():
        row_copy(1, "tx").start()

    for to in partners[0]:
        box_copy(2, to, tx).wait_send()
    arrive_all(3)

    @pl.when(ty > 0)
    def _():
        row_copy(0, "ty").wait_send()
        row_copy(1, "ty").wait_recv()

    @pl.when(ty < NY - 1)
    def _():
        row_copy(1, "ty").wait_send()
        row_copy(0, "ty").wait_recv()

    @pl.when(ty == NY - 1)
    def _():
        row_copy(1, "tx").wait()

    edges[0] = rows_in[0]
    edges[0, TIERS : TIERS + 1] = jnp.where(ty > 0, rows_in[0, TIERS : TIERS + 1], 0.0)
    turn = 127 - lax.broadcasted_iota(i32, (24, LANES), 1)
    upper = rows_in[1]
    flipped = [jnp.take_along_axis(upper[:, LANES * v : LANES * v + LANES], turn, axis=1) for v in (3, 2, 1, 0)]
    edges[1] = jnp.where(ty == NY - 1, jnp.concatenate(flipped, axis=1), upper)

    for to in partners[0]:
        box_copy(3, to, tx).wait_send()


def finish(field, lap, depth, least, rims, edges, field_out, lap_out, ends, late, sem):
    middle = pl.ds(BAND, CJ - 2 * BAND)
    half = TIERS // 2
    copies = [pltpu.make_async_copy(field.at[pl.ds(half * n, half)], field_out.at[pl.ds(half * n, half)], sem.at[n]) for n in (0, 1)]
    copies.append(pltpu.make_async_copy(lap.at[pl.ds(0, DONE), middle], lap_out.at[pl.ds(0, DONE), middle], sem.at[2]))
    for copy in copies:
        copy.start()

    def outer(ref, tier, band):
        row = edges[1 if band else 0, tier : tier + 1]
        return around(ref, band, tier, rims, **{"above" if band else "below": row})

    for place, band in enumerate((0, LAST)):
        here, *others = outer(depth, TIERS, band)
        bounds = [jnp.minimum(here, other) for other in others]
        for tier in range(TIERS):
            ends[place, tier] = divergence(outer(field.at[tier], tier, band), bounds, tier)
        copies.append(pltpu.make_async_copy(ends.at[place], lap_out.at[:, pl.ds(BAND * band, BAND)], sem.at[3 + place]))
        copies[-1].start()
    for part in range((TIERS - DONE) // 2):
        for tier in (DONE + 2 * part, DONE + 2 * part + 1):
            for band in INNER:
                bounds = [least[side, BAND * band : BAND * band + BAND] for side in range(4)]
                late[tier - DONE, BAND * (band - 1) : BAND * band] = divergence(around(field.at[tier], band, tier, rims), bounds, tier)
        two = pl.ds(DONE + 2 * part, 2)
        copies.append(pltpu.make_async_copy(late.at[pl.ds(2 * part, 2)], lap_out.at[two, middle], sem.at[5 + part]))
        copies[-1].start()
    for copy in copies:
        copy.wait()


def on_device(warmth, salt, tally):
    hbm = pl.BlockSpec(memory_space=pltpu.HBM)
    vmem = pl.BlockSpec(memory_space=pltpu.VMEM)
    held = pl.pallas_call(
        exchange,
        out_shape=(
            pltpu.VMEM((TIERS, CJ, CI), f32),
            pltpu.VMEM((TIERS, CJ, CI), f32),
            pltpu.VMEM((CJ, CI), f32),
            pltpu.VMEM((4, CJ, CI), f32),
            pltpu.VMEM((NX, BAND, LANES), f32),
            pltpu.VMEM((2, 24, CI), f32),
        ),
        in_specs=[hbm] * 3,
        out_specs=(vmem,) * 6,
        scratch_shapes=[
            pltpu.VMEM((TIERS, BAND, COLS), f32),
            pltpu.VMEM((TIERS, BAND, COLS), f32),
            pltpu.VMEM((BAND, COLS), i32),
            pltpu.VMEM((2 * NX, BOX, LANES), f32),
            pltpu.VMEM((NX, ROWS, LANES), i32),
            pltpu.VMEM((NX, KEPT, LANES), i32),
            pltpu.VMEM((NX, ROWS, LANES), i32),
            pltpu.VMEM((NX, ROWS, LANES), i32),
            pltpu.VMEM((NX, BAND, LANES), f32),
            pltpu.VMEM((2, BAND, LANES), f32),
            pltpu.VMEM((2, 24, CI), f32),
            pltpu.VMEM((2, 24, CI), f32),
            pltpu.SemaphoreType.DMA((2 * CHUNKS + 1,)),
            pltpu.SemaphoreType.DMA((CHUNKS + 1, NX)),
            pltpu.SemaphoreType.DMA((CHUNKS + 1, NX)),
            pltpu.SemaphoreType.DMA((NX,)),
            pltpu.SemaphoreType.DMA((2,)),
            pltpu.SemaphoreType.DMA((2,)),
            pltpu.SemaphoreType.DMA((2,)),
        ],
        compiler_params=pltpu.CompilerParams(collective_id=0, has_side_effects=True, vmem_limit_bytes=48 * 2**20),
        name="exchange",
    )(warmth, salt, tally)
    return pl.pallas_call(
        finish,
        out_shape=(jax.ShapeDtypeStruct((TIERS, CJ, CI), f32),) * 2,
        in_specs=[vmem] * 6,
        out_specs=(hbm,) * 2,
        scratch_shapes=[
            pltpu.VMEM((2, TIERS, BAND, CI), f32),
            pltpu.VMEM((TIERS - DONE, CJ - 2 * BAND, CI), f32),
            pltpu.SemaphoreType.DMA((5 + (TIERS - DONE) // 2,)),
        ],
        compiler_params=pltpu.CompilerParams(vmem_limit_bytes=16 * 2**20),
        name="finish",
    )(*held)


def solution(mesh):
    placed = (P(None, ("ty", "tx"), None), P(None, ("ty", "tx"), None), P(("ty", "tx"), None))
    return jax.shard_map(
        on_device,
        mesh=mesh,
        in_specs=placed,
        out_specs=(P(None, "ty", "tx"), P(None, "ty", "tx")),
        check_vma=False,
    )
```

```python
import jax
import jax.numpy as jnp
from jax import lax
from jax.experimental import pallas as pl
from jax.experimental.pallas import tpu as pltpu
from jax.sharding import PartitionSpec as P

therm_coef = 0.1655
haline_coef = 0.76554
cabbel_coef = 0.05952
haline_second = 0.00054914
thermo_press = 0.0001497
haline_press = 1.109e-05
cross_coef = 0.0024341

MESH = pl.DeviceIdType.MESH
TIERS = 16
BAND = 8
CJ = 128
CI = 512
NX = 16
NY = 8
COLS = NX * CI
LANES = 128
ROWS = BAND * CI // LANES
KEPT = 24
SPARE = (ROWS - KEPT) * LANES
CUTS = (0, 6, 10, 14, 16)
CHUNKS = len(CUTS) - 1
EARLY = CUTS[-2]
DONE = CUTS[-3]
RIM = ROWS + CUTS[1] * KEPT
BOX = ROWS + TIERS * KEPT + BAND
INNER = range(1, NX - 1)
LAST = NX - 1
ZFIRST = ((0, 2), (2, 2), (0, 1), (1, 1), (3, 3), (0, 3), (2, 1), (2, 3), (1, 2), (3, 2), (1, 3), (3, 1), (2, 0), (1, 0), (3, 0), (0, 0))
FARFIRST = ((2, 2), (2, 1), (2, 3), (1, 2), (3, 2), (1, 1), (3, 3), (1, 3), (3, 1), (2, 0), (0, 2), (1, 0), (3, 0), (0, 1), (0, 3), (0, 0))
ORDERS = (ZFIRST, FARFIRST, FARFIRST, FARFIRST, ZFIRST)
f32 = jnp.float32
i32 = jnp.int32


def density(warmth, salt, tier):
    depth = 5.0 + 10.0 * tier
    a = warmth - 10.0
    b = salt - 35.0
    heat = (-therm_coef * (1.0 + thermo_press * depth)) - (0.5 * therm_coef * cabbel_coef) * a - cross_coef * b
    salty = (haline_coef * (1.0 - haline_press * depth)) - (0.5 * haline_coef * haline_second) * b
    return heat * a + salty * b


def partner_of(tx, step, chunk, way=1):
    dy = jnp.int32(0)
    dz = jnp.int32(0)
    for number, (far_y, far_z) in enumerate(ORDERS[chunk]):
        dy = jnp.where(step == number, far_y, dy)
        dz = jnp.where(step == number, far_z, dz)
    return ((tx // 4 + way * dy) & 3) * 4 + ((tx + way * dz) & 3)


def row_of(tier):
    return ROWS + KEPT * tier + (BAND if tier >= CUTS[1] else 0)


def as_rows(block):
    return jnp.concatenate([block[:, LANES * v : LANES * v + LANES] for v in range(CI // LANES)], axis=0)


def as_block(rows):
    return jnp.concatenate([rows[BAND * v : BAND * v + BAND] for v in range(CI // LANES)], axis=1)


def land_counts(land):
    one = lax.broadcasted_iota(i32, (LANES, 2 * LANES), 0)
    two = lax.broadcasted_iota(i32, (LANES, 2 * LANES), 1)
    ahead = jnp.where(jnp.logical_or(two >= LANES, one < two), 1.0, 0.0).astype(jnp.bfloat16)
    both = jnp.dot(land.astype(jnp.bfloat16), ahead, preferred_element_type=f32)
    one = lax.broadcasted_iota(i32, (ROWS, ROWS), 0)
    two = lax.broadcasted_iota(i32, (ROWS, ROWS), 1)
    above = jnp.where(two < one, 1.0, 0.0).astype(jnp.bfloat16)
    start = jnp.dot(above, both[:, LANES:].astype(jnp.bfloat16), preferred_element_type=f32)
    cell = jnp.minimum(start + both[:, :LANES], float(SPARE))
    return jnp.minimum(start, float(SPARE)).astype(i32), cell.astype(i32)


def squeeze(state, bits, axis, roll):
    size = state.shape[axis]
    for bit in range(bits):
        flag = 256 << bit
        ahead = roll(state, size - (1 << bit), axis)
        stay = jnp.where((state & flag) != 0, 0, state)
        state = jnp.where((ahead & flag) != 0, ahead, stay)
    return state


def packing(tally, roll):
    start, cell = land_counts(jnp.where(tally > 0, 0.0, 1.0))
    lane = lax.broadcasted_iota(i32, (ROWS, LANES), 1)
    row = lax.broadcasted_iota(i32, (ROWS, LANES), 0)
    state = jnp.where(tally > 0, ((cell - start) << 8) | 128 | lane, 0)
    state = squeeze(state, 7, 1, roll) & 255
    state = jnp.take_along_axis(state, (lane + start) & 127, axis=1)
    back = (start + lane) >> 7
    rows = jnp.where(state >= 128, (back << 8) | row, 0)
    rows = squeeze(rows, 4, 0, roll) & 31
    return state & 127, rows[:KEPT]


def unpacking(tally):
    start, cell = land_counts(jnp.where(tally > 0, 0.0, 1.0))
    lane = lax.broadcasted_iota(i32, (ROWS, LANES), 1)
    row = lax.broadcasted_iota(i32, (ROWS, LANES), 0)
    return row - ((start + lane) >> 7), (lane - cell) & 127


def pack(rows, lane_from, row_from):
    moved = jnp.take_along_axis(rows, lane_from, axis=1)
    parts = []
    for w in range(KEPT // BAND):
        at = row_from[BAND * w : BAND * w + BAND]
        low = jnp.take_along_axis(moved[BAND * w : BAND * w + BAND], at & 7, axis=0)
        high = jnp.take_along_axis(moved[BAND * w + BAND : BAND * w + 2 * BAND], at & 7, axis=0)
        parts.append(jnp.where(at >= BAND * (w + 1), high, low))
    return jnp.concatenate(parts, axis=0)


def unpack(kept, row_from, lane_from):
    parts = []
    for v in range(ROWS // BAND):
        at = row_from[BAND * v : BAND * v + BAND]
        low = None if v == 0 else jnp.take_along_axis(kept[BAND * v - BAND : BAND * v], at & 7, axis=0)
        high = None if v == KEPT // BAND else jnp.take_along_axis(kept[BAND * v : BAND * v + BAND], at & 7, axis=0)
        if low is None or high is None:
            parts.append(high if low is None else low)
        else:
            parts.append(jnp.where(at >= BAND * v, high, low))
    return jnp.take_along_axis(jnp.concatenate(parts, axis=0), lane_from, axis=1)


def around(ref, band, tier, rims, above=None, below=None):
    lanes = lax.broadcasted_iota(i32, (BAND, LANES), 1)
    row = lax.broadcasted_iota(i32, (BAND, CI), 0)
    here = ref[BAND * band : BAND * band + BAND]
    if above is None:
        above = pltpu.roll(ref[BAND * band + BAND : BAND * band + 2 * BAND], BAND - 1, 0)
    if below is None:
        below = pltpu.roll(ref[BAND * band - BAND : BAND * band], 1, 0)
    north = jnp.where(row == BAND - 1, above, pltpu.roll(here, BAND - 1, 0))
    south = jnp.where(row == 0, below, pltpu.roll(here, 1, 0))
    rim = rims[band]
    east = pltpu.roll(here, CI - 1, 1)
    east_rim = pltpu.roll(rim, 127 - 32 - tier, 1)
    east = jnp.concatenate([east[:, : CI - LANES], jnp.where(lanes == 127, east_rim, east[:, CI - LANES :])], 1)
    west = pltpu.roll(here, 1, 1)
    west_rim = pltpu.roll(rim, LANES - tier, 1)
    west = jnp.concatenate([jnp.where(lanes == 0, west_rim, west[:, :LANES]), west[:, LANES:]], 1)
    return here, north, south, east, west


def divergence(cells, bounds, level):
    here, *others = cells
    total = None
    for bound, other in zip(bounds, others):
        term = jnp.where(bound > level, other - here, 0.0)
        total = term if total is None else total + term
    return total


def exchange(
    warmth, salt, tally, out, lap, depth, least, rims, edges,
    heat, brine, bottom, boxes, pack_lane, pack_row, lane_back, row_back, brink_out, brink_in, rows_out, rows_in,
    in_sem, send_sem, recv_sem, brink_ssem, brink_rsem, row_ssem, row_rsem,
):
    ty = lax.axis_index("ty")
    tx = lax.axis_index("tx")
    outer = jnp.logical_or(tx == 0, tx == LAST)
    barrier = pltpu.get_barrier_semaphore()
    loads = [pltpu.make_async_copy(tally, bottom, in_sem.at[2 * CHUNKS])]
    for chunk in range(CHUNKS):
        part = pl.ds(CUTS[chunk], CUTS[chunk + 1] - CUTS[chunk])
        loads.append(pltpu.make_async_copy(warmth.at[part], heat.at[part], in_sem.at[2 * chunk]))
        loads.append(pltpu.make_async_copy(salt.at[part], brine.at[part], in_sem.at[2 * chunk + 1]))
    loads[0].start()
    for step in range(1, NX):
        pl.semaphore_signal(barrier, inc=1, device_id={"tx": (tx + step) & LAST}, device_id_type=MESH)

    @pl.when(ty > 0)
    def _():
        pl.semaphore_signal(barrier, inc=1, device_id={"ty": ty - 1}, device_id_type=MESH)

    @pl.when(ty < NY - 1)
    def _():
        pl.semaphore_signal(barrier, inc=1, device_id={"ty": ty + 1}, device_id_type=MESH)

    for load in loads[1:]:
        load.start()
    lanes = lax.broadcasted_iota(i32, (BAND, LANES), 1)
    partners = [[((tx // 4 + dy) & 3) * 4 + ((tx + dz) & 3) for dy, dz in order[:-1]] for order in ORDERS]

    def box_copy(chunk, to, source):
        part = pl.ds(0, ROWS)
        if chunk < CHUNKS:
            first = RIM if chunk == 1 else row_of(CUTS[chunk])
            part = pl.ds(first, row_of(CUTS[chunk + 1] - 1) + KEPT - first)
        return pltpu.make_async_remote_copy(
            src_ref=boxes.at[to, part], dst_ref=boxes.at[NX + source, part],
            send_sem=send_sem.at[chunk, to], recv_sem=recv_sem.at[chunk, source],
            device_id={"tx": to}, device_id_type=MESH,
        )

    def brink_copy(to, source):
        side = jnp.where(source == 0, 0, 1)
        return pltpu.make_async_remote_copy(
            src_ref=brink_out.at[to], dst_ref=brink_in.at[side],
            send_sem=brink_ssem.at[to], recv_sem=brink_rsem.at[side],
            device_id={"tx": to}, device_id_type=MESH,
        )

    def find(to):
        at = pl.ds(pl.multiple_of(to * CI, CI), CI)
        lane_from, row_from = packing(as_rows(bottom[:, at]), pltpu.roll)
        pack_lane[to] = lane_from
        pack_row[to] = row_from
        return lane_from, row_from

    def make_rim(to):
        west = pl.ds(pl.multiple_of(((to * CI) + COLS - LANES) & (COLS - 1), LANES), LANES)
        east = pl.ds(pl.multiple_of(((to * CI) + CI) & (COLS - 1), LANES), LANES)
        rim = pltpu.roll(bottom[:, west].astype(f32), TIERS + 1, 1)
        rim = jnp.where(lanes == 32 + TIERS, pltpu.roll(bottom[:, east].astype(f32), 32 + TIERS, 1), rim)
        for tier in range(TIERS):
            low = density(heat[tier, :, west], brine[tier, :, west], tier)
            high = density(heat[tier, :, east], brine[tier, :, east], tier)
            rim = jnp.where(lanes == tier, pltpu.roll(low, tier + 1, 1), rim)
            rim = jnp.where(lanes == 32 + tier, pltpu.roll(high, 32 + tier, 1), rim)
        boxes[jnp.where(to == tx, NX + to, to), RIM : RIM + BAND] = rim

    def make(first, last, step):
        to = partner_of(tx, step, CUTS.index(first))
        slot = jnp.where(step == LAST, NX + to, to)
        at = pl.ds(pl.multiple_of(to * CI, CI), CI)
        lane_from, row_from = find(to) if first == 0 else (pack_lane[to], pack_row[to])
        for tier in range(first, last):
            value = density(heat[tier, :, at], brine[tier, :, at], tier)
            boxes[slot, row_of(tier) : row_of(tier) + KEPT] = pack(as_rows(value), lane_from, row_from)
            if tier >= EARLY:
                brink = jnp.where(tx == 0, value[:1], value[BAND - 1 :])
                for v in range(CI // LANES):
                    place = (tier - EARLY) * (CI // LANES) + v
                    brink_out[to, place : place + 1] = brink[:, LANES * v : LANES * v + LANES]

    def make_two(first, last, pair):
        for n in (0, 1):
            make(first, last, 2 * pair + n)

    def wait_loads(chunk):
        loads[1 + 2 * chunk].wait()
        loads[2 + 2 * chunk].wait()

    def make_and_send(first, last, sends, before):
        def one(pair, carry):
            make_two(first, last, pair)

            @pl.when(pair > 0)
            def _():
                if sends is not None:
                    box_copy(sends, partner_of(tx, 2 * pair - 2, sends), tx).start()
                    box_copy(sends, partner_of(tx, 2 * pair - 1, sends), tx).start()

            @pl.when(pair == 0)
            def _():
                if before is not None:
                    box_copy(before, partners[before][LAST - 1], tx).start()

            return carry

        lax.fori_loop(0, NX // 2, one, 0)

    def take_tally(to, carry):
        at = pl.ds(pl.multiple_of(to * CI, CI), CI)
        boxes[jnp.where(to == tx, NX + to, to), :ROWS] = as_rows(bottom[:, at]).astype(f32)
        return carry

    loads[0].wait()
    lax.fori_loop(0, NX, take_tally, 0, unroll=4)
    neighbours = jnp.where(ty > 0, 1, 0) + jnp.where(ty < NY - 1, 1, 0)
    pl.semaphore_wait(barrier, NX - 1 + neighbours)
    for to in partners[CHUNKS]:
        box_copy(CHUNKS, to, tx).start()
    wait_loads(0)
    make_and_send(CUTS[0], CUTS[1], 0, None)
    for chunk in range(1, CHUNKS):
        wait_loads(chunk)

    def rim_two(pair, carry):
        make_rim(2 * pair)
        make_rim(2 * pair + 1)
        return carry

    lax.fori_loop(0, NX // 2, rim_two, 0)
    box_copy(0, partners[0][LAST - 1], tx).start()
    make_and_send(CUTS[1], CUTS[2], 1, None)
    make_and_send(CUTS[2], CUTS[3], 2, 1)
    make_and_send(CUTS[3], CUTS[4], None, 2)

    @pl.when(outer)
    def _():
        brink_in[jnp.where(tx == 0, 0, 1)] = brink_out[tx]
        for to in partners[0]:
            brink_copy(to, tx).start()

    for to in partners[3]:
        box_copy(3, to, tx).start()

    def arrive(chunk, source):
        @pl.when(source != tx)
        def _():
            if chunk == 0:
                box_copy(CHUNKS, source, source).wait_recv()
            box_copy(chunk, source, source).wait_recv()

        rows = pl.ds(pl.multiple_of(source * BAND, BAND), BAND)
        deep = boxes[NX + source, :ROWS]
        if chunk == 0:
            row_from, lane_from = unpacking(deep)
            row_back[source] = row_from
            lane_back[source] = lane_from
            deep = as_block(deep)
            depth[rows] = deep
        else:
            row_from = row_back[source]
            lane_from = lane_back[source]
            deep = as_block(deep)
        if chunk == 1:
            rims[source] = boxes[NX + source, RIM : RIM + BAND]
        for tier in range(CUTS[chunk], CUTS[chunk + 1]):
            kept = boxes[NX + source, row_of(tier) : row_of(tier) + KEPT]
            out[tier, rows] = jnp.where(deep > tier, as_block(unpack(kept, row_from, lane_from)), 0.0)

    def arrive_all(chunk):
        def one(step, carry):
            arrive(chunk, partner_of(tx, (step + LAST) & LAST, chunk, -1))
            return carry

        lax.fori_loop(0, NX, one, 0)

    def laplace(chunk):
        def one(tier, carry):
            for band in INNER:
                rows = slice(BAND * band, BAND * band + BAND)
                bounds = [least[side, rows] for side in range(4)]
                lap[tier, rows] = divergence(around(out.at[tier], band, tier, rims), bounds, tier.astype(f32))
            return carry

        lax.fori_loop(CUTS[chunk], CUTS[chunk + 1], one, 0)

    arrive_all(0)
    arrive_all(1)

    for band in INNER:
        here, *others = around(depth, band, TIERS, rims)
        for side, other in enumerate(others):
            least[side, BAND * band : BAND * band + BAND] = jnp.minimum(here, other)
    laplace(0)
    laplace(1)

    arrive_all(2)
    for side, at in ((0, 0), (1, CJ - 1)):
        @pl.when(tx != (LAST if side else 0))
        def _():
            brink_copy(LAST if side else 0, LAST if side else 0).wait_recv()

        for tier in range(EARLY):
            rows_out[side, tier : tier + 1] = out[tier, at : at + 1]
        rows_out[side, TIERS : TIERS + 1] = depth[at : at + 1]
        for place in range((TIERS - EARLY) * CI // LANES):
            tier, v = EARLY + place // (CI // LANES), place % (CI // LANES)
            rows_out[side, tier : tier + 1, LANES * v : LANES * v + LANES] = brink_in[side, place : place + 1]

    def row_copy(side, along):
        place = 1 - side if along == "ty" else 1
        if along == "ty":
            device = {"ty": jnp.minimum(ty + 1, NY - 1) if side else jnp.maximum(ty - 1, 0)}
        else:
            device = {"tx": LAST - tx}
        return pltpu.make_async_remote_copy(
            src_ref=rows_out.at[side], dst_ref=rows_in.at[place], send_sem=row_ssem.at[side], recv_sem=row_rsem.at[place],
            device_id=device, device_id_type=MESH,
        )

    @pl.when(outer)
    def _():
        for to in partners[0]:
            brink_copy(to, tx).wait_send()

    for to in partners[0]:
        for chunk in (CHUNKS, 0, 1):
            box_copy(chunk, to, tx).wait_send()

    @pl.when(ty > 0)
    def _():
        row_copy(0, "ty").start()

    @pl.when(ty < NY - 1)
    def _():
        row_copy(1, "ty").start()

    @pl.when(ty == NY - 1)
    def _():
        row_copy(1, "tx").start()

    for to in partners[0]:
        box_copy(2, to, tx).wait_send()
    arrive_all(3)

    @pl.when(ty > 0)
    def _():
        row_copy(0, "ty").wait_send()
        row_copy(1, "ty").wait_recv()

    @pl.when(ty < NY - 1)
    def _():
        row_copy(1, "ty").wait_send()
        row_copy(0, "ty").wait_recv()

    @pl.when(ty == NY - 1)
    def _():
        row_copy(1, "tx").wait()

    edges[0] = rows_in[0]
    edges[0, TIERS : TIERS + 1] = jnp.where(ty > 0, rows_in[0, TIERS : TIERS + 1], 0.0)
    turn = 127 - lax.broadcasted_iota(i32, (24, LANES), 1)
    upper = rows_in[1]
    flipped = [jnp.take_along_axis(upper[:, LANES * v : LANES * v + LANES], turn, axis=1) for v in (3, 2, 1, 0)]
    edges[1] = jnp.where(ty == NY - 1, jnp.concatenate(flipped, axis=1), upper)

    for to in partners[0]:
        box_copy(3, to, tx).wait_send()


def finish(field, lap, depth, least, rims, edges, field_out, lap_out, ends, late, sem):
    middle = pl.ds(BAND, CJ - 2 * BAND)
    half = TIERS // 2
    copies = [pltpu.make_async_copy(field.at[pl.ds(half * n, half)], field_out.at[pl.ds(half * n, half)], sem.at[n]) for n in (0, 1)]
    copies.append(pltpu.make_async_copy(lap.at[pl.ds(0, DONE), middle], lap_out.at[pl.ds(0, DONE), middle], sem.at[2]))
    for copy in copies:
        copy.start()

    def outer(ref, tier, band):
        row = edges[1 if band else 0, tier : tier + 1]
        return around(ref, band, tier, rims, **{"above" if band else "below": row})

    for place, band in enumerate((0, LAST)):
        here, *others = outer(depth, TIERS, band)
        bounds = [jnp.minimum(here, other) for other in others]
        for tier in range(TIERS):
            ends[place, tier] = divergence(outer(field.at[tier], tier, band), bounds, tier)
        copies.append(pltpu.make_async_copy(ends.at[place], lap_out.at[:, pl.ds(BAND * band, BAND)], sem.at[3 + place]))
        copies[-1].start()
    for part in range((TIERS - DONE) // 2):
        for tier in (DONE + 2 * part, DONE + 2 * part + 1):
            for band in INNER:
                bounds = [least[side, BAND * band : BAND * band + BAND] for side in range(4)]
                late[tier - DONE, BAND * (band - 1) : BAND * band] = divergence(around(field.at[tier], band, tier, rims), bounds, tier)
        two = pl.ds(DONE + 2 * part, 2)
        copies.append(pltpu.make_async_copy(late.at[pl.ds(2 * part, 2)], lap_out.at[two, middle], sem.at[5 + part]))
        copies[-1].start()
    for copy in copies:
        copy.wait()


def on_device(warmth, salt, tally):
    hbm = pl.BlockSpec(memory_space=pltpu.HBM)
    vmem = pl.BlockSpec(memory_space=pltpu.VMEM)
    held = pl.pallas_call(
        exchange,
        out_shape=(
            pltpu.VMEM((TIERS, CJ, CI), f32),
            pltpu.VMEM((TIERS, CJ, CI), f32),
            pltpu.VMEM((CJ, CI), f32),
            pltpu.VMEM((4, CJ, CI), f32),
            pltpu.VMEM((NX, BAND, LANES), f32),
            pltpu.VMEM((2, 24, CI), f32),
        ),
        in_specs=[hbm] * 3,
        out_specs=(vmem,) * 6,
        scratch_shapes=[
            pltpu.VMEM((TIERS, BAND, COLS), f32),
            pltpu.VMEM((TIERS, BAND, COLS), f32),
            pltpu.VMEM((BAND, COLS), i32),
            pltpu.VMEM((2 * NX, BOX, LANES), f32),
            pltpu.VMEM((NX, ROWS, LANES), i32),
            pltpu.VMEM((NX, KEPT, LANES), i32),
            pltpu.VMEM((NX, ROWS, LANES), i32),
            pltpu.VMEM((NX, ROWS, LANES), i32),
            pltpu.VMEM((NX, BAND, LANES), f32),
            pltpu.VMEM((2, BAND, LANES), f32),
            pltpu.VMEM((2, 24, CI), f32),
            pltpu.VMEM((2, 24, CI), f32),
            pltpu.SemaphoreType.DMA((2 * CHUNKS + 1,)),
            pltpu.SemaphoreType.DMA((CHUNKS + 1, NX)),
            pltpu.SemaphoreType.DMA((CHUNKS + 1, NX)),
            pltpu.SemaphoreType.DMA((NX,)),
            pltpu.SemaphoreType.DMA((2,)),
            pltpu.SemaphoreType.DMA((2,)),
            pltpu.SemaphoreType.DMA((2,)),
        ],
        compiler_params=pltpu.CompilerParams(collective_id=0, has_side_effects=True, vmem_limit_bytes=48 * 2**20),
        name="exchange",
    )(warmth, salt, tally)
    return pl.pallas_call(
        finish,
        out_shape=(jax.ShapeDtypeStruct((TIERS, CJ, CI), f32),) * 2,
        in_specs=[vmem] * 6,
        out_specs=(hbm,) * 2,
        scratch_shapes=[
            pltpu.VMEM((2, TIERS, BAND, CI), f32),
            pltpu.VMEM((TIERS - DONE, CJ - 2 * BAND, CI), f32),
            pltpu.SemaphoreType.DMA((5 + (TIERS - DONE) // 2,)),
        ],
        compiler_params=pltpu.CompilerParams(vmem_limit_bytes=16 * 2**20),
        name="finish",
    )(*held)


def solution(mesh):
    placed = (P(None, ("ty", "tx"), None), P(None, ("ty", "tx"), None), P(("ty", "tx"), None))
    return jax.shard_map(
        on_device,
        mesh=mesh,
        in_specs=placed,
        out_specs=(P(None, "ty", "tx"), P(None, "ty", "tx")),
        check_vma=False,
    )
```
